32 devices in a mesh: seq: 8 (over z, y), head: 4 (over x, core).
Axes of the slice: x: 2, y: 2, z: 4, core: 2. Of those that a mesh axis runs over, the one named last changes fastest.
Arguments:
- residual: bfloat16 [4096, 3072], P('seq', 'head'), may hold values from -6 to 6
- q_self: bfloat16 [4096, 3072], P('seq', 'head'), may hold values from -6 to 6
- k_self: bfloat16 [4096, 3072], P('seq', 'head'), may hold values from -6 to 6
- v_self: bfloat16 [4096, 3072], P('seq', 'head'), may hold values from -6 to 6
- w_out: bfloat16 [3072, 3072], P('head'), may hold values from -0.109375 to 0.109375
- norm_gain: float32 [3072], replicated, may hold values from 0.5 to 1.5
- w_query: bfloat16 [3072, 3072], P('seq', 'head')
- w_cache: bfloat16 [3072, 2048], P('seq', 'head')
- block_doc: int32 [8], replicated, may hold values from 0 to 2, never falling along the last dimension, each value on 1 to 4 neighbouring positions
- tail_len: int32 [8], replicated, may hold values from 1 to 512
Outputs:
- hidden: bfloat16 [4096, 3072], P('seq', 'head')
- cross_context: bfloat16 [4096, 3072], P('seq', 'head')
The draws below stay inside these ranges and needn't reach their ends.
Inputs may be any that keep to these rules, and one draw needn't show every extreme that they name: block_doc never falls along the blocks; each document covers 1 to 4 consecutive blocks, and some document covers exactly 4. `tail_len`: read only for the last block of a document.
All inputs are finite; a program needn't handle non-finite values.
Results may differ from the reference program's by a relative error of at most 0.0078.
Values may be sent and summed in bfloat16 or wider, within the bound.
No kernel may reach another device: no remote copies, remote signals or barrier semaphores. Data moves between devices by JAX's collectives and lax.ppermute only.
A program may use at most 128 MiB of HBM per device.

```python
import math
import jax
import jax.numpy as jnp
import numpy as np
from jax import lax

D = 3072
HEADS = 24
KV_HEADS = 8
HEAD_DIM = 128
TOK_DEV = 512
WINDOW = 2048
DOC_MAX = 2560
WIN_BLOCKS = 4
DOC_BLOCKS = 5
NBLK = 8
TOKENS = 4096
SPAN_MAX = 4
DOC_COUNT = 3
N_HEAD = 4


def sign_vector(key, length):
    return jnp.where(jax.random.randint(key, (length,), 0, 2) == 0, -1.0, 1.0).astype(jnp.float32)


def picked_rows(key):
    every = max(2, TOK_DEV // 64)
    return jax.random.randint(key, (TOKENS,), 0, TOK_DEV) < every


def base_noise(key, shape):
    return jax.random.normal(jax.random.fold_in(key, 3), shape, jnp.float32)


def self_operand(key, member):
    width = HEADS * HEAD_DIM
    plan = jax.random.fold_in(key, 9001)
    picked = picked_rows(jax.random.fold_in(plan, 1))
    pattern = sign_vector(jax.random.fold_in(plan, 2), width)
    strength = jax.random.uniform(jax.random.fold_in(plan, 3), (TOKENS,), jnp.float32, 3.0, 5.5)
    spread = 0.4
    noise = base_noise(jax.random.fold_in(key, member), (TOKENS, width))
    aligned = strength[:, None] * pattern[None, :] + spread * noise
    mixed = jnp.where(picked[:, None], aligned, noise)
    return jnp.clip(mixed, -6.0, 6.0).astype(jnp.bfloat16)


def draw_q_self(key, part):
    return self_operand(key, 11)


def draw_k_self(key, part):
    return self_operand(key, 12)


def cross_patterns(key):
    plan = jax.random.fold_in(key, 9002)
    return (sign_vector(jax.random.fold_in(plan, 1), D), sign_vector(jax.random.fold_in(plan, 2), HEAD_DIM))


def draw_residual(key, part):
    feature_sign = cross_patterns(key)[0]
    plan = jax.random.fold_in(key, 9003)
    picked = picked_rows(jax.random.fold_in(plan, 1))
    strength = jax.random.uniform(jax.random.fold_in(plan, 2), (TOKENS,), jnp.float32, 2.0, 4.5)
    noise = base_noise(jax.random.fold_in(key, 13), (TOKENS, D))
    aligned = strength[:, None] * feature_sign[None, :] + 0.3 * noise
    mixed = jnp.where(picked[:, None], aligned, noise)
    return jnp.clip(mixed, -6.0, 6.0).astype(jnp.bfloat16)


def scaled_noise(key, columns):
    limit = 6.0 * D ** (-0.5)
    return jnp.clip(base_noise(key, (D, columns)) * D ** (-0.5), -limit, limit)


def draw_w_query(key, part):
    feature_sign, head_sign = cross_patterns(key)
    width = HEADS * HEAD_DIM
    noise = scaled_noise(jax.random.fold_in(key, 14), width)
    amounts = jax.random.uniform(jax.random.fold_in(key, 9005), (HEADS,), jnp.float32, 14.5, 24.5)
    columns = (amounts[:, None] * head_sign[None, :]).reshape(width)
    plant = feature_sign[:, None] * columns[None, :] / (D * HEAD_DIM ** 0.25)
    return (noise + plant).astype(jnp.bfloat16)


def draw_w_cache(key, part):
    feature_sign, head_sign = cross_patterns(key)
    group = KV_HEADS // N_HEAD
    width = 2 * KV_HEADS * HEAD_DIM
    noise = scaled_noise(jax.random.fold_in(key, 15), width)
    key_part = jnp.broadcast_to(16.0 * head_sign, (N_HEAD, group, HEAD_DIM))
    columns = jnp.stack([key_part, jnp.zeros_like(key_part)], axis=1).reshape(width)
    plant = feature_sign[:, None] * columns[None, :] / (D * HEAD_DIM ** 0.25)
    return (noise + plant).astype(jnp.bfloat16)


def with_ends(drawn, own_key, least, top_value):
    place = [jax.random.randint(jax.random.fold_in(own_key, axis), (), 0, length) for axis, length in enumerate(drawn.shape)]
    longest = drawn.shape.index(max(drawn.shape))
    next_to = place[:longest] + [(place[longest] + 1) % drawn.shape[longest]] + place[longest + 1:]
    return drawn.at[tuple(place)].set(least).at[tuple(next_to)].set(top_value)


def block_levels(own_key, shape, cuts, least, largest):
    factor_of = 1.0
    for axis_at, blocks in cuts:
        steps = jax.random.uniform(jax.random.fold_in(jax.random.fold_in(own_key, 6), axis_at), (blocks,), jnp.float32, least / len(cuts), largest / len(cuts))
        factor_of = factor_of * jnp.repeat(jnp.exp(steps), shape[axis_at] // blocks).reshape((-1,) + (1,) * (len(shape) - 1 - axis_at))
    return factor_of


def profile(count, total, most, lean):
    loads = [(1 << 20) // math.isqrt(standing ** lean) + 1 for standing in range(2, count + 1)]
    rest, holding = total - most - (count - 1), [1] * (count - 1)
    while rest > 0:
        free = [i for i in range(count - 1) if holding[i] < most]
        mass, remaining = sum([loads[i] for i in free]), rest
        for i in free:
            addition = min(most - holding[i], max(1, remaining * loads[i] // mass), rest)
            holding[i] = holding[i] + addition
            rest = rest - addition
    return np.array([most] + holding)


def uneven(own_key, amount, total, reach, lean):
    if amount == 2:
        one = jax.random.randint(own_key, (), max(1, total - reach), min(reach, total - 1) + 1)
        return jnp.stack([one, total - one])
    sizes = jnp.asarray(profile(amount, total, reach, lean), jnp.int32)
    pairs = (amount - 1) // 2
    giver, receiver = sizes[1:1 + 2 * pairs:2], sizes[2:2 + 2 * pairs:2]
    slack = jnp.minimum(giver - 1, reach - receiver)
    shifted = jax.random.randint(jax.random.fold_in(own_key, 1), (pairs,), 0, 1 << 20) % (slack + 1)
    sizes = sizes.at[1:1 + 2 * pairs:2].set(giver - shifted).at[2:2 + 2 * pairs:2].set(receiver + shifted)
    return sizes[jax.random.permutation(jax.random.fold_in(own_key, 2), amount)]


def bell_draw(stream_key, extent, scale, most, cuts=(), kind=jnp.bfloat16):
    entries = scale * jax.random.normal(stream_key, extent, jnp.float32)
    if cuts:
        entries = entries * block_levels(stream_key, extent, cuts, -0.22, 0.18)
    return jnp.clip(entries, -most, most).astype(kind)


def setup_inputs(seed: int = 0) -> dict:
    arg_keys = jax.random.split(jax.random.key(seed), 11)
    residual = draw_residual(jax.random.fold_in(arg_keys[10], 71), 0)
    q_self = draw_q_self(jax.random.fold_in(arg_keys[10], 71), 0)
    k_self = draw_k_self(jax.random.fold_in(arg_keys[10], 71), 0)
    v_self = bell_draw(arg_keys[3], (TOKENS, HEADS * HEAD_DIM), 1.0, 6.0, ((0, 8), (1, 4)))
    w_out = bell_draw(arg_keys[4], (HEADS * HEAD_DIM, D), (HEADS * HEAD_DIM) ** -0.5, 0.109375, ((0, 4),))
    norm_gain = jnp.clip(1.0 + 0.1 * jax.random.normal(arg_keys[5], (D,), jnp.float32), 0.5, 1.5)
    w_query = draw_w_query(jax.random.fold_in(arg_keys[10], 71), 0)
    w_cache = draw_w_cache(jax.random.fold_in(arg_keys[10], 71), 0)
    block_doc = jnp.searchsorted(jnp.cumsum(uneven(arg_keys[8], DOC_COUNT, NBLK, SPAN_MAX, 2)), jnp.arange(NBLK), side="right").astype(jnp.int32)
    tail_len = with_ends(jax.random.randint(arg_keys[9], (NBLK,), 1, TOK_DEV + 1), jax.random.fold_in(arg_keys[9], 1), 1, TOK_DEV).astype(jnp.int32)
    return dict(residual=residual, q_self=q_self, k_self=k_self, v_self=v_self, w_out=w_out, norm_gain=norm_gain, w_query=w_query, w_cache=w_cache, block_doc=block_doc, tail_len=tail_len)


EPSILON = 1e-06

def block_valid(block_doc, tail_len, tok_rows):
    following = jnp.concatenate([block_doc[1:], jnp.full((1,), -1, jnp.int32)])
    closing = following != block_doc
    within = jnp.arange(tok_rows, dtype=jnp.int32)
    return jnp.logical_or(jnp.logical_not(closing)[:, None], within[None, :] < tail_len[:, None])

def permitted(query_block, key_blocks, block_doc, valid_tokens, tok_rows, reach_tokens):
    inside = key_blocks >= 0
    safe_blocks = jnp.maximum(key_blocks, 0)
    own_doc = jnp.take(block_doc, query_block)
    same_doc = jnp.logical_and(inside, jnp.take(block_doc, safe_blocks) == own_doc)
    live_keys = jnp.logical_and(same_doc[:, None], jnp.take(valid_tokens, safe_blocks, axis=0))
    within = jnp.arange(tok_rows, dtype=jnp.int32)
    query_pos = query_block * tok_rows + within
    key_pos = (key_blocks[:, None] * tok_rows + within[None, :]).reshape(-1)
    distance = query_pos[:, None] - key_pos[None, :]
    near = jnp.logical_and(distance >= 0, distance < reach_tokens)
    return jnp.logical_and(near, live_keys.reshape(-1)[None, :])

def attend(queries, keys, values, allowed):
    row_count, head_count, head_dim = queries.shape
    group_size = head_count // keys.shape[1]
    scaling = 1.0 / math.sqrt(head_dim)

    def one_head(head_index):
        query_head = lax.dynamic_index_in_dim(queries, head_index, 1, keepdims=False)
        key_head = lax.dynamic_index_in_dim(keys, head_index // group_size, 1, keepdims=False)
        value_head = lax.dynamic_index_in_dim(values, head_index // group_size, 1, keepdims=False)
        scores = lax.dot_general(query_head, key_head, (((1,), (1,)), ((), ())), preferred_element_type=jnp.float32) * scaling
        scores = jnp.where(allowed, scores, -1e+30)
        row_peak = lax.optimization_barrier(jnp.max(scores, axis=1, keepdims=True))
        weights = jnp.exp(scores - row_peak)
        row_total = lax.optimization_barrier(jnp.sum(weights, axis=1, keepdims=True))
        blended = jnp.dot(weights.astype(jnp.bfloat16), value_head, preferred_element_type=jnp.float32)
        return (blended / row_total).astype(jnp.bfloat16)
    per_head = lax.map(one_head, jnp.arange(head_count, dtype=jnp.int32))
    return jnp.transpose(per_head, (1, 0, 2)).reshape(row_count, head_count * head_dim)

def reference(residual, q_self, k_self, v_self, w_out, norm_gain, w_query, w_cache, block_doc, tail_len):
    valid_tokens = block_valid(block_doc, tail_len, TOK_DEV)
    width_all = HEADS * HEAD_DIM
    win_rows = WIN_BLOCKS * TOK_DEV
    key_pad = jnp.concatenate([jnp.zeros((win_rows, width_all), jnp.bfloat16), k_self], axis=0)
    value_pad = jnp.concatenate([jnp.zeros((win_rows, width_all), jnp.bfloat16), v_self], axis=0)

    def self_block(block_index):
        row_start = block_index * TOK_DEV
        queries = lax.dynamic_slice_in_dim(q_self, row_start, TOK_DEV, 0).reshape(TOK_DEV, HEADS, HEAD_DIM)
        keys = lax.dynamic_slice_in_dim(key_pad, row_start, win_rows + TOK_DEV, 0).reshape(-1, HEADS, HEAD_DIM)
        values = lax.dynamic_slice_in_dim(value_pad, row_start, win_rows + TOK_DEV, 0).reshape(-1, HEADS, HEAD_DIM)
        key_blocks = block_index - WIN_BLOCKS + jnp.arange(WIN_BLOCKS + 1, dtype=jnp.int32)
        allowed = permitted(block_index, key_blocks, block_doc, valid_tokens, TOK_DEV, WINDOW)
        return attend(queries, keys, values, allowed)
    context = lax.map(self_block, jnp.arange(NBLK, dtype=jnp.int32)).reshape(TOKENS, width_all)
    projected = jnp.dot(context, w_out, preferred_element_type=jnp.float32)
    hidden = (residual.astype(jnp.float32) + projected).astype(jnp.bfloat16)
    wide = hidden.astype(jnp.float32)
    mean_square = lax.optimization_barrier(jnp.mean(wide * wide, axis=1, keepdims=True))
    normed = (wide * lax.rsqrt(mean_square + EPSILON) * norm_gain).astype(jnp.bfloat16)
    cross_queries = jnp.dot(normed, w_query, preferred_element_type=jnp.float32).astype(jnp.bfloat16)
    cache_rows = jnp.dot(normed, w_cache, preferred_element_type=jnp.float32).astype(jnp.bfloat16)
    cache_rows = cache_rows.reshape(TOKENS, N_HEAD, 2, KV_HEADS // N_HEAD, HEAD_DIM)
    cache_keys = cache_rows[:, :, 0].reshape(TOKENS, KV_HEADS * HEAD_DIM)
    cache_values = cache_rows[:, :, 1].reshape(TOKENS, KV_HEADS * HEAD_DIM)
    doc_rows = (DOC_BLOCKS - 1) * TOK_DEV
    cache_key_pad = jnp.concatenate([jnp.zeros((doc_rows, KV_HEADS * HEAD_DIM), jnp.bfloat16), cache_keys], axis=0)
    cache_value_pad = jnp.concatenate([jnp.zeros((doc_rows, KV_HEADS * HEAD_DIM), jnp.bfloat16), cache_values], axis=0)

    def cross_block(block_index):
        row_start = block_index * TOK_DEV
        queries = lax.dynamic_slice_in_dim(cross_queries, row_start, TOK_DEV, 0).reshape(TOK_DEV, HEADS, HEAD_DIM)
        keys = lax.dynamic_slice_in_dim(cache_key_pad, row_start, doc_rows + TOK_DEV, 0).reshape(-1, KV_HEADS, HEAD_DIM)
        values = lax.dynamic_slice_in_dim(cache_value_pad, row_start, doc_rows + TOK_DEV, 0).reshape(-1, KV_HEADS, HEAD_DIM)
        key_blocks = block_index - DOC_BLOCKS + 1 + jnp.arange(DOC_BLOCKS, dtype=jnp.int32)
        allowed = permitted(block_index, key_blocks, block_doc, valid_tokens, TOK_DEV, DOC_MAX)
        return attend(queries, keys, values, allowed)
    cross_context = lax.map(cross_block, jnp.arange(NBLK, dtype=jnp.int32)).reshape(TOKENS, width_all)
    return (hidden, cross_context)
```

```python
import functools
import math

import jax
import jax.numpy as jnp
from jax import lax
from jax.experimental import pallas as pl
from jax.experimental.pallas import tpu as pltpu
from jax.sharding import PartitionSpec as P

HEAD_DIM = 128
WINDOW = 2048
EPSILON = 1e-06
LOG2E = 1.4426950408889634


def moved(block, axis, size, target):
    route = [(i, target(i)) for i in range(size)]
    route = [(i, j) for i, j in route if j is not None and 0 <= j < size]
    return lax.ppermute(block, axis, route)


def attend_kernel(
    place_ref, doc_ref, tail_ref, q_ref, *refs, slots, heads, group, q_tile, reach
):
    kv_refs = refs[: len(slots)]
    o_ref, m_ref, l_ref, acc_ref = refs[len(slots) :]
    rows = q_ref.shape[0]
    blocks = doc_ref.shape[0]
    kv_heads = heads // group
    factor = LOG2E / math.sqrt(HEAD_DIM)
    here = place_ref[0]
    own_doc = doc_ref[here]
    after = jnp.minimum(here + 1, blocks - 1)
    closing = jnp.logical_or(here == blocks - 1, doc_ref[after] != own_doc)
    live = jnp.where(closing, tail_ref[here], rows)

    def scores(kv_ref, t, h):
        q = q_ref[pl.ds(t, q_tile), h * HEAD_DIM : (h + 1) * HEAD_DIM]
        g = h // group
        k = kv_ref[:, g * HEAD_DIM : (g + 1) * HEAD_DIM]
        return lax.dot_general(q, k, (((1,), (1,)), ((), ())), preferred_element_type=jnp.float32)

    def values(kv_ref, h):
        g = kv_heads + h // group
        return kv_ref[:, g * HEAD_DIM : (g + 1) * HEAD_DIM]

    def tiles(step):
        def body(i, carry):
            step(pl.multiple_of(i * q_tile, q_tile))
            return carry

        lax.fori_loop(0, rows // q_tile, body, 0)

    def first(t):
        kv_ref = kv_refs[0]
        row = t + lax.broadcasted_iota(jnp.int32, (q_tile, rows), 0)
        col = lax.broadcasted_iota(jnp.int32, (q_tile, rows), 1)
        keep = jnp.logical_and(col <= row, col < live)
        for h in range(heads):
            s = jnp.where(keep, scores(kv_ref, t, h), -1e30)
            m = jnp.max(s, axis=1, keepdims=True)
            p = jnp.exp2((s - m) * factor)
            m_ref[h, pl.ds(t, q_tile), :] = jnp.broadcast_to(m, (q_tile, HEAD_DIM))
            l_ref[h, pl.ds(t, q_tile), :] = jnp.broadcast_to(
                jnp.sum(p, axis=1, keepdims=True), (q_tile, HEAD_DIM)
            )
            acc_ref[h, pl.ds(t, q_tile), :] = jnp.dot(
                p.astype(jnp.bfloat16), values(kv_ref, h), preferred_element_type=jnp.float32
            )

    def later(kv_ref, back):
        def step(t):
            if back * rows + rows - 1 >= reach:
                row = t + lax.broadcasted_iota(jnp.int32, (q_tile, rows), 0)
                col = lax.broadcasted_iota(jnp.int32, (q_tile, rows), 1)
                keep = back * rows + row - col < reach
            else:
                keep = None
            for h in range(heads):
                s = scores(kv_ref, t, h)
                if keep is not None:
                    s = jnp.where(keep, s, -1e30)
                m_old = m_ref[h, pl.ds(t, q_tile), :]
                m = jnp.maximum(m_old, jnp.max(s, axis=1, keepdims=True))
                shrink = jnp.exp2((m_old - m) * factor)
                p = jnp.exp2((s - m[:, :1]) * factor)
                m_ref[h, pl.ds(t, q_tile), :] = m
                l_ref[h, pl.ds(t, q_tile), :] = l_ref[h, pl.ds(t, q_tile), :] * shrink + jnp.sum(
                    p, axis=1, keepdims=True
                )
                acc_ref[h, pl.ds(t, q_tile), :] = acc_ref[
                    h, pl.ds(t, q_tile), :
                ] * shrink + jnp.dot(
                    p.astype(jnp.bfloat16), values(kv_ref, h), preferred_element_type=jnp.float32
                )

        return step

    tiles(first)
    for kv_ref, (even, odd) in zip(kv_refs[1:], slots[1:]):
        parity = lax.rem(here, 2)
        for back, only in ((even, 0), (odd, 1)):
            if back is None or (even == odd and only == 1):
                continue
            source = here - back
            wanted = jnp.logical_and(source >= 0, doc_ref[jnp.maximum(source, 0)] == own_doc)
            if even != odd:
                wanted = jnp.logical_and(wanted, parity == only)
            span = back

            @pl.when(wanted)
            def _(kv_ref=kv_ref, span=span):
                tiles(later(kv_ref, span))

    for h in range(heads):
        o_ref[:, h * HEAD_DIM : (h + 1) * HEAD_DIM] = (acc_ref[h] / l_ref[h]).astype(jnp.bfloat16)


def attend(place, block_doc, tail_len, queries, column_block, heads, kv_list, slots, reach):
    rows, width = kv_list[0].shape
    kv_heads = width // (2 * HEAD_DIM)
    wide = heads * HEAD_DIM
    smem = pl.BlockSpec(memory_space=pltpu.SMEM)
    whole = pl.BlockSpec((rows, width), lambda i: (0, 0))
    return pl.pallas_call(
        functools.partial(
            attend_kernel,
            slots=slots,
            heads=heads,
            group=heads // kv_heads,
            q_tile=min(256, rows),
            reach=reach,
        ),
        grid=(1,),
        out_shape=jax.ShapeDtypeStruct((rows, wide), jnp.bfloat16),
        in_specs=[smem, smem, smem, pl.BlockSpec((rows, wide), lambda i: (0, column_block))]
        + [whole] * len(kv_list),
        out_specs=pl.BlockSpec((rows, wide), lambda i: (0, 0)),
        scratch_shapes=[pltpu.VMEM((heads, rows, HEAD_DIM), jnp.float32)] * 3,
        compiler_params=pltpu.CompilerParams(vmem_limit_bytes=48 * 2**20),
        name="attend",
    )(place, block_doc, tail_len, queries, *kv_list)


def project_kernel(*refs, parts, blocks):
    residual_ref = refs[0]
    context_refs = refs[1 : 1 + parts * blocks]
    w_refs = refs[1 + parts * blocks : 1 + parts * blocks + blocks]
    o_ref = refs[-1]
    total = residual_ref[...].astype(jnp.float32)
    depth = context_refs[0].shape[1]
    for part in range(parts):
        for block in range(blocks):
            total += jnp.dot(
                context_refs[part * blocks + block][...],
                w_refs[block][part * depth : (part + 1) * depth, :],
                preferred_element_type=jnp.float32,
            )
    o_ref[...] = total.astype(jnp.bfloat16)


def norm_kernel(place_ref, gain_ref, *refs, near):
    hidden_refs, o_ref = refs[:-1], refs[-1]
    wide = hidden_refs[0].shape[1]
    total = 0.0
    for ref in hidden_refs:
        x = ref[...].astype(jnp.float32)
        total += jnp.sum(x * x, axis=1, keepdims=True)
    scale = lax.rsqrt(total / (wide * len(hidden_refs)) + EPSILON)
    for step, ref in enumerate(hidden_refs):
        at = pl.multiple_of(near(place_ref[0], step) * wide, wide)
        x = ref[...].astype(jnp.float32)
        o_ref[:, pl.ds(at, wide)] = (x * scale * gain_ref[:, pl.ds(at, wide)]).astype(jnp.bfloat16)


def columns_kernel(order_ref, normed_ref, *refs):
    w_refs, o_ref = refs[:-1], refs[-1]
    depth = w_refs[0].shape[0]
    total = 0.0
    for step, ref in enumerate(w_refs):
        at = pl.multiple_of(order_ref[step] * depth, depth)
        total += jnp.dot(
            normed_ref[:, pl.ds(at, depth)], ref[...], preferred_element_type=jnp.float32
        )
    o_ref[...] = total.astype(jnp.bfloat16)


def simple_call(kernel, out_shape, scalars, arrays, name):
    return pl.pallas_call(
        kernel,
        out_shape=out_shape,
        in_specs=[pl.BlockSpec(memory_space=pltpu.SMEM)] * len(scalars)
        + [pl.BlockSpec(memory_space=pltpu.VMEM)] * len(arrays),
        out_specs=pl.BlockSpec(memory_space=pltpu.VMEM),
        compiler_params=pltpu.CompilerParams(vmem_limit_bytes=56 * 2**20),
        name=name,
    )(*scalars, *arrays)


def local(
    residual,
    q_self,
    k_self,
    v_self,
    w_out,
    norm_gain,
    w_query,
    w_cache,
    block_doc,
    tail_len,
    *,
    seq,
    head,
    span,
    paired,
):
    rows, own = residual.shape
    local_heads = q_self.shape[1] // HEAD_DIM
    local_kv = w_cache.shape[1] // (2 * HEAD_DIM)
    place = lax.axis_index("seq").astype(jnp.int32)
    lane = lax.axis_index("head").astype(jnp.int32)
    place1, lane1 = place[None], lane[None]

    def along(block, target):
        return moved(block, "seq", seq, target)

    def across(block, step):
        return moved(block, "head", head, lambda i: i ^ step)

    even = lambda i: i % 2 == 0

    def spread(block):
        if not paired:
            return [along(block, lambda i, d=d: i + d) for d in range(1, span)]
        far = along(block, lambda i: i + 2)
        near = along(block, lambda i: i + 1 if even(i) else None)
        swap = along(far, lambda i: i ^ 1)
        last = along(swap, lambda i: i + 2 if even(i) else None)
        return [far, near, swap, last]

    if paired:
        slots = ((0, 0), (2, 2), (None, 1), (1, 3), (3, None))
    else:
        slots = tuple((d, d) for d in range(span))

    parts = local_heads // 2
    per = local_heads // parts
    width = per * HEAD_DIM
    kv_parts = []
    for c in range(parts):
        cols = slice(c * width, (c + 1) * width)
        own_kv = jnp.concatenate([k_self[:, cols], v_self[:, cols]], axis=1)
        kv_parts.append([own_kv] + spread(own_kv))

    w_blocks = []
    for step in range(head):
        piece = lax.dynamic_slice_in_dim(w_out, (lane ^ step) * own, own, 1)
        w_blocks.append(piece if step == 0 else across(piece, step))

    def gathered(w):
        if not paired:
            whole = lax.all_gather(w, "seq", axis=0, tiled=True)
            return [whole]
        pieces = [w, along(w, lambda i: i ^ 1)]
        ring = list(pieces)
        for distance in range(1, seq // 2):
            if distance <= seq // 4:
                ring = [along(p, lambda i: (i - 2) % seq) for p in ring]
                pieces += ring
            else:
                pieces += [
                    along(p, lambda i: (i + 2 * (seq // 2 - distance)) % seq) for p in pieces[:2]
                ]
        return pieces

    if paired:
        order = [(place ^ y) + 2 * distance for distance in range(seq // 2) for y in (0, 1)]
        order = jnp.stack([lax.rem(o, seq) for o in order])
    else:
        order = jnp.zeros((1,), jnp.int32)
    cache_w = gathered(w_cache)
    query_w = gathered(w_query)

    contexts = []
    for c in range(parts):
        mine = attend(
            place1, block_doc, tail_len, q_self, c, per, kv_parts[c], slots, WINDOW
        )
        pair = [mine, across(mine, 2)]
        other = [across(p, 1) for p in pair]
        contexts += [pair[0], other[0], pair[1], other[1]]
    hidden = simple_call(
        functools.partial(project_kernel, parts=parts, blocks=head),
        jax.ShapeDtypeStruct((rows, own), jnp.bfloat16),
        [],
        [residual, *contexts, *w_blocks],
        "project",
    )
    pair = [hidden, across(hidden, 2)]
    other = [across(p, 1) for p in pair]
    normed = simple_call(
        functools.partial(norm_kernel, near=lambda at, step: at ^ step),
        jax.ShapeDtypeStruct((rows, own * head), jnp.bfloat16),
        [lane1],
        [norm_gain[None, :], pair[0], other[0], pair[1], other[1]],
        "norm",
    )
    cache = simple_call(
        columns_kernel,
        jax.ShapeDtypeStruct((rows, w_cache.shape[1]), jnp.bfloat16),
        [order],
        [normed, *cache_w],
        "cache",
    )
    history = [cache] + spread(cache)
    cross_queries = simple_call(
        columns_kernel,
        jax.ShapeDtypeStruct((rows, w_query.shape[1]), jnp.bfloat16),
        [order],
        [normed, *query_w],
        "queries",
    )
    cross_context = attend(
        place1,
        block_doc,
        tail_len,
        cross_queries,
        0,
        local_heads,
        history,
        slots,
        rows * span,
    )
    return (hidden, cross_context)


def solution(mesh):
    seq, head = mesh.shape["seq"], mesh.shape["head"]
    span = min(5, seq // 2)
    in_specs = (
        P("seq", "head"),
        P("seq", "head"),
        P("seq", "head"),
        P("seq", "head"),
        P("head", None),
        P(),
        P("seq", "head"),
        P("seq", "head"),
        P(),
        P(),
    )
    out_specs = (P("seq", "head"), P("seq", "head"))
    body = functools.partial(local, seq=seq, head=head, span=span, paired=span == 4)
    return jax.shard_map(body, mesh=mesh, in_specs=in_specs, out_specs=out_specs, check_vma=False)
```

```python
import functools
import math

import jax
import jax.numpy as jnp
from jax import lax
from jax.experimental import pallas as pl
from jax.experimental.pallas import tpu as pltpu
from jax.sharding import PartitionSpec as P


HEAD_DIM = 128
WINDOW = 2048
EPSILON = 1e-06
SELF_TILE = 256
VMEM_LIMIT = 24 * 2**20
CROSS_TILE = 256
LOG2E = 1.4426950408889634


def moved(block, axis, size, target):
    route = [(i, target(i)) for i in range(size)]
    route = [(i, j) for i, j in route if j is not None and 0 <= j < size]
    return lax.ppermute(block, axis, route)


def attend_kernel(
    place_ref, doc_ref, tail_ref, *refs, arrays, groups, sources, q_sources, tile, mode
):
    count = len(sources) * len(groups)
    q_refs, refs = refs[:arrays], refs[arrays:]
    kv_refs, refs = refs[:count], refs[count:]
    if mode == "finish":
        ml_in, acc_in, *old_refs = refs[: 2 + arrays]
        o_refs = refs[2 + arrays :]
    else:
        o_refs, states = refs[:arrays], refs[arrays:]
    rows = q_refs[0].shape[0]
    blocks = doc_ref.shape[0]
    factor = LOG2E / math.sqrt(HEAD_DIM)
    here = place_ref[0]
    parity = lax.rem(here, 2)

    def lanes(at):
        if isinstance(at, int):
            return slice(at * HEAD_DIM, (at + 1) * HEAD_DIM)
        return pl.ds(pl.multiple_of(at * HEAD_DIM, HEAD_DIM), HEAD_DIM)

    def block_of(source):
        if source[0] == "back":
            return here - source[1]
        if source[0] == "pair":
            return here + 1 - 2 * parity - source[1]
        return here - parity - 1 - source[1]

    def joined(key_block, query_block):
        safe = jnp.maximum(key_block, 0)
        wanted = jnp.logical_and(key_block >= 0, key_block < query_block)
        return jnp.logical_and(wanted, doc_ref[safe] == doc_ref[query_block])

    def live_rows(block):
        after = jnp.minimum(block + 1, blocks - 1)
        closing = jnp.logical_or(block == blocks - 1, doc_ref[after] != doc_ref[block])
        return jnp.where(closing, tail_ref[block], rows)

    def soften(q, spans, before):
        k = jnp.concatenate([k for k, _, _, _ in spans], axis=0)
        v = jnp.concatenate([v for _, v, _, _ in spans], axis=0)
        v = jnp.concatenate([v, jnp.ones(v.shape, v.dtype)], axis=1)
        s_all = lax.dot_general(q, k, (((1,), (1,)), ((), ())), preferred_element_type=jnp.float32)
        parts, at = [], 0
        m = None if before is None else before[0]
        for k, _, keep, open_span in spans:
            s = s_all[:, at : at + k.shape[0]]
            at += k.shape[0]
            if keep is not None:
                s = jnp.where(keep, s, -1e30)
            peak = jnp.max(s, axis=1, keepdims=True)
            if open_span is not None:
                peak = jnp.where(open_span, peak, -1e30)
            m = peak if m is None else jnp.maximum(m, peak)
            parts.append((s, open_span))
        weights = []
        for s, open_span in parts:
            top = m if open_span is None else jnp.where(open_span, m, 1e30)
            weights.append(jnp.exp2((s - top) * factor).astype(jnp.bfloat16))
        acc = jnp.dot(
            jnp.concatenate(weights, axis=1), v, preferred_element_type=jnp.float32
        )
        if before is not None:
            shrink = jnp.exp2((before[0] - m) * factor)
            return m, acc[:, HEAD_DIM:] + before[1] * shrink, acc[:, :HEAD_DIM] + before[2] * shrink
        return m, acc[:, HEAD_DIM:], acc[:, :HEAD_DIM]

    def state_lane(index):
        return lax.broadcasted_iota(jnp.int32, (tile, HEAD_DIM), 1) == index

    def over_heads(body):
        for g, (heads, shared) in enumerate(groups):
            slots = kv_refs[g * len(sources) : (g + 1) * len(sources)]
            kv_heads = slots[0].shape[1] // (2 * HEAD_DIM)

            def one(h, carry, g=g, heads=heads, shared=shared, slots=slots, kv_heads=kv_heads):
                at = 0 if shared else h

                def pick(slot, keys):
                    return slot[:keys, lanes(at)], slot[:keys, lanes(kv_heads + at)]

                body(slots, g * heads + h, pick)
                return carry

            lax.fori_loop(0, heads, one, 0)

    def begin(slots, head, pick):
        def visit(n, extra):
            query_block = block_of(q_sources[n])
            live = live_rows(query_block)
            for t in range(0, rows, tile):
                keys = t + tile
                row = t + lax.broadcasted_iota(jnp.int32, (tile, keys), 0)
                col = lax.broadcasted_iota(jnp.int32, (tile, keys), 1)
                keep = jnp.logical_and(col <= row, col < live)
                spans = [(*pick(slots[sources.index(q_sources[n])], keys), keep, None)]
                for slot, source in zip(slots, sources):
                    if source not in q_sources or source == extra:
                        spans.append((*pick(slot, rows), None, joined(block_of(source), query_block)))
                m, total, acc = soften(q_refs[n][t : t + tile, lanes(head)], spans, None)
                o_refs[n][t : t + tile, lanes(head)] = (acc / total).astype(jnp.bfloat16)
                if arrays == 1 or extra is None:
                    ml_out, acc_out = states
                    acc_out[t : t + tile, lanes(head)] = acc
                    kept = jnp.where(state_lane(2 * head), m, ml_out[t : t + tile, :])
                    ml_out[t : t + tile, :] = jnp.where(state_lane(2 * head + 1), total, kept)

        if arrays == 1:
            visit(0, None)
            return
        for first in (0, 1):

            @pl.when(parity == first)
            def _(first=first):
                visit(first, None)
                visit(1 - first, q_sources[first])

    def finish(slots, head, pick):
        for n, (q_ref, old_ref, o_ref) in enumerate(zip(q_refs, old_refs, o_refs)):

            def go(q_ref=q_ref, o_ref=o_ref, n=n):
                query_block = block_of(q_sources[n])
                for t in range(0, rows, tile):
                    ml = ml_in[t : t + tile, :]
                    before = [
                        jnp.sum(jnp.where(state_lane(2 * head + i), ml, 0.0), axis=1, keepdims=True)
                        for i in (0, 1)
                    ]
                    before.append(acc_in[t : t + tile, lanes(head)])
                    spans = [
                        (*pick(slot, rows), None, joined(block_of(source), query_block))
                        for slot, source in zip(slots, sources)
                    ]
                    _, total, acc = soften(q_ref[t : t + tile, lanes(head)], spans, before)
                    o_ref[t : t + tile, lanes(head)] = (acc / total).astype(jnp.bfloat16)

            if arrays == 1:
                go()
            else:
                pl.when(parity == n)(go)

                @pl.when(parity != n)
                def _(old_ref=old_ref, o_ref=o_ref):
                    o_ref[:, lanes(head)] = old_ref[:, lanes(head)]

    if mode == "begin":
        states[0][...] = jnp.zeros(states[0].shape, jnp.float32)
    over_heads(finish if mode == "finish" else begin)


def attend(scalars, q_list, kv_list, groups, sources, q_sources, tile, mode, state=()):
    rows, wide = q_list[0].shape
    arrays = len(q_list)
    smem = pl.BlockSpec(memory_space=pltpu.SMEM)
    vmem = pl.BlockSpec(memory_space=pltpu.VMEM)
    heads = sum(g[0] for g in groups)
    operands = [*q_list, *kv_list, *state]
    out_shape = [jax.ShapeDtypeStruct((rows, wide), jnp.bfloat16)] * arrays
    if mode == "begin":
        out_shape += [
            jax.ShapeDtypeStruct((rows, d * HEAD_DIM), jnp.float32) for d in (1, heads)
        ]
    return pl.pallas_call(
        functools.partial(
            attend_kernel,
            arrays=arrays,
            groups=tuple(groups),
            sources=tuple(sources),
            q_sources=tuple(q_sources),
            tile=min(tile, rows),
            mode=mode,
        ),
        out_shape=out_shape,
        in_specs=[smem] * len(scalars) + [vmem] * len(operands),
        out_specs=[vmem] * len(out_shape),
        compiler_params=pltpu.CompilerParams(vmem_limit_bytes=VMEM_LIMIT),
        name="attend",
    )(*scalars, *operands)


def project_call(places, base, pieces, w_blocks, first, out_type):
    rows, own = base.shape
    half = own // 2

    def kernel(places_ref, base_ref, *refs):
        near_refs, w_refs = refs[: len(pieces)], refs[len(pieces) : -2]
        o_ref, context_ref = refs[-2:]
        side = lax.rem(places_ref[0], 2)
        for step, ref in enumerate(near_refs):
            block, other = divmod(step, 2)
            at = block * own + (side if other == 0 else 1 - side) * half
            context_ref[:, pl.ds(pl.multiple_of(at, half), half)] = ref[...]
        total = base_ref[...].astype(jnp.float32)
        for block, w_ref in enumerate(w_refs):
            total += jnp.dot(
                context_ref[:, block * own : (block + 1) * own],
                w_ref[...],
                preferred_element_type=jnp.float32,
            )
        o_ref[...] = total.astype(o_ref.dtype)

    whole = lambda a: pl.BlockSpec(a.shape, lambda i, places_ref: (0, 0))
    corner = pl.BlockSpec((own, own), lambda i, places_ref: (0, places_ref[1] if first else 0))
    return pl.pallas_call(
        kernel,
        grid_spec=pltpu.PrefetchScalarGridSpec(
            num_scalar_prefetch=1,
            grid=(1,),
            in_specs=[whole(a) for a in (base, *pieces)]
            + [corner]
            + [whole(w) for w in w_blocks[1:]],
            out_specs=whole(base),
            scratch_shapes=[pltpu.VMEM((rows, own * len(w_blocks)), jnp.bfloat16)],
        ),
        out_shape=jax.ShapeDtypeStruct((rows, own), out_type),
        compiler_params=pltpu.CompilerParams(vmem_limit_bytes=VMEM_LIMIT),
        name="project",
    )(places, base, *pieces, *w_blocks)


def norm_into(lane, gain_ref, hidden_refs, normed_ref):
    wide = hidden_refs[0].shape[1]
    total = 0.0
    for ref in hidden_refs:
        x = ref[...].astype(jnp.float32)
        total += jnp.sum(x * x, axis=1, keepdims=True)
    scale = lax.rsqrt(total / (wide * len(hidden_refs)) + EPSILON)
    for step, ref in enumerate(hidden_refs):
        at = pl.multiple_of((lane ^ step) * wide, wide)
        x = ref[...].astype(jnp.float32)
        normed_ref[:, pl.ds(at, wide)] = (x * scale * gain_ref[:, pl.ds(at, wide)]).astype(
            jnp.bfloat16
        )


def fetch(place_ref, pieces, columns, buffer, sems, rings):
    z, y = place_ref[0] // 2, lax.rem(place_ref[0], 2)
    depth = buffer.shape[1] // 2
    order = []
    for k in range(rings):
        order.append(lax.rem(z - k + rings, rings))
        for t in (0, 1):
            rows = pl.ds(pl.multiple_of((y ^ t) * depth, depth), depth)

            def begin(name, slot=2 * k + t, k=k, rows=rows):
                ref, base = pieces[name]
                pltpu.make_async_copy(
                    ref.at[:, columns.start - base : columns.stop - base],
                    buffer.at[k, rows],
                    sems.at[slot],
                ).start()

            if k == 0:
                begin(("w", 0, t))
            else:

                @pl.when(z >= k)
                def _(k=k, t=t, begin=begin):
                    begin(("up", k, t))

                @pl.when(z < k)
                def _(k=k, t=t, begin=begin):
                    begin(("down", rings - k, t))

    return order


def gather_dot(normed_ref, order, pieces, columns, buffer, sems):
    total = 0.0
    first = pieces[("w", 0, 0)][0]
    depth = first.shape[0]
    for k, block in enumerate(order):
        for t in (0, 1):
            pltpu.make_async_copy(
                first.at[:, 0 : columns.stop - columns.start],
                buffer.at[k, pl.ds(t * depth, depth)],
                sems.at[2 * k + t],
            ).wait()
        at = pl.multiple_of(block * 2 * depth, 2 * depth)
        total += jnp.dot(
            normed_ref[:, pl.ds(at, 2 * depth)], buffer[k], preferred_element_type=jnp.float32
        )
    return total


def cache_call(place1, lane1, gain, hiddens, pieces, width, rings):
    names = list(pieces)
    rows, own = hiddens[0].shape
    depth = pieces[("w", 0, 0)][0].shape[0]
    groups = width // (2 * HEAD_DIM)
    columns = slice(0, width)

    def kernel(place_ref, lane_ref, gain_ref, *refs):
        hidden_refs = refs[: len(hiddens)]
        piece_refs = refs[len(hiddens) : len(hiddens) + len(names)]
        normed_ref, *cache_refs = refs[len(hiddens) + len(names) : -2]
        buffer, sems = refs[-2:]
        at = {n: (r, pieces[n][1]) for n, r in zip(names, piece_refs)}
        order = fetch(place_ref, at, columns, buffer, sems, rings)
        norm_into(lane_ref[0], gain_ref, hidden_refs, normed_ref)
        total = gather_dot(normed_ref, order, at, columns, buffer, sems)
        for g, ref in enumerate(cache_refs):
            for part in (0, 1):
                c = (part * groups + g) * HEAD_DIM
                ref[:, part * HEAD_DIM : (part + 1) * HEAD_DIM] = total[
                    :, c : c + HEAD_DIM
                ].astype(jnp.bfloat16)

    vmem = pl.BlockSpec(memory_space=pltpu.VMEM)
    smem = pl.BlockSpec(memory_space=pltpu.SMEM)
    return pl.pallas_call(
        kernel,
        out_shape=[jax.ShapeDtypeStruct((rows, own * len(hiddens)), jnp.bfloat16)]
        + [jax.ShapeDtypeStruct((rows, 2 * HEAD_DIM), jnp.bfloat16)] * groups,
        in_specs=[smem, smem, vmem]
        + [vmem] * len(hiddens)
        + [pl.BlockSpec(memory_space=pl.ANY)] * len(names),
        out_specs=[vmem] * (1 + groups),
        scratch_shapes=[
            pltpu.VMEM((rings, 2 * depth, width), jnp.bfloat16),
            pltpu.SemaphoreType.DMA((2 * rings,)),
        ],
        compiler_params=pltpu.CompilerParams(vmem_limit_bytes=VMEM_LIMIT),
        name="cache",
    )(place1, lane1, gain, *hiddens, *[pieces[n][0] for n in names])


def query_call(place1, normed, pieces, start, width, rings):
    names = list(pieces)
    rows = normed.shape[0]
    depth = pieces[("w", 0, 0)][0].shape[0]
    columns = slice(start, start + width)

    def kernel(place_ref, normed_ref, *refs):
        piece_refs = refs[: len(names)]
        o_ref, buffer, sems = refs[len(names) :]
        at = {n: (r, pieces[n][1]) for n, r in zip(names, piece_refs)}
        order = fetch(place_ref, at, columns, buffer, sems, rings)
        o_ref[...] = gather_dot(normed_ref, order, at, columns, buffer, sems).astype(jnp.bfloat16)

    vmem = pl.BlockSpec(memory_space=pltpu.VMEM)
    return pl.pallas_call(
        kernel,
        out_shape=jax.ShapeDtypeStruct((rows, width), jnp.bfloat16),
        in_specs=[pl.BlockSpec(memory_space=pltpu.SMEM), vmem]
        + [pl.BlockSpec(memory_space=pl.ANY)] * len(names),
        out_specs=vmem,
        scratch_shapes=[
            pltpu.VMEM((rings, 2 * depth, width), jnp.bfloat16),
            pltpu.SemaphoreType.DMA((2 * rings,)),
        ],
        compiler_params=pltpu.CompilerParams(vmem_limit_bytes=VMEM_LIMIT),
        name="queries",
    )(place1, normed, *[pieces[n][0] for n in names])


def paired_layer(
    residual,
    q_self,
    k_self,
    v_self,
    w_out,
    norm_gain,
    w_query,
    w_cache,
    block_doc,
    tail_len,
    *,
    seq,
    head,
):
    _, own = residual.shape
    half = own // 2
    parts = half // HEAD_DIM
    rings = seq // 2
    groups = w_cache.shape[1] // (2 * HEAD_DIM)
    place = lax.axis_index("seq").astype(jnp.int32)
    lane = lax.axis_index("head").astype(jnp.int32)
    side = lax.rem(place, 2)
    place1, lane1 = place[None], lane[None]

    def send(block, axis, target, source=None):
        size = seq if axis == "seq" else head
        return moved(
            block, axis, size, lambda i: target(i) if source is None or source(i) else None
        )

    up = lambda i: i + 2
    swap = lambda i: i ^ 1
    column = lambda a, at, size: lax.dynamic_slice_in_dim(a, at, size, 1)

    def kv_of(which):
        at = which * half
        return jnp.concatenate([column(k_self, at, half), column(v_self, at, half)], axis=1)

    mine, theirs = kv_of(side), kv_of(1 - side)
    q_mine = column(q_self, side * half, half)
    q_theirs = column(q_self, (1 - side) * half, half)
    above = send(mine, "seq", up)
    near = send(theirs, "seq", swap)
    across = send(near, "seq", up)
    odd = jnp.where(side == 1, above, across)
    far = send(odd, "seq", up, lambda i: i >= 2)
    q_near = send(q_theirs, "seq", swap)

    w_blocks = [w_out]
    late = lax.optimization_barrier(w_out)
    for step in (2, 1, 3):
        source = late if step == 1 else w_out
        piece = lax.dynamic_slice_in_dim(source, (lane ^ step) * own, own, 1)
        w_blocks.append(send(piece, "head", lambda i: i ^ step))

    wide = w_cache.shape[1]
    tables = []
    for name, w, base in (("c", w_cache, 0), ("q", w_query, wide)):
        table = {("w", 0, 0): (w, base)}
        table[("w", 0, 1)] = (send(w, "seq", swap), base)
        high = w
        for k in range(1, rings):
            if name == "q":
                high = send(high, "seq", up, lambda i: i // 2 >= k - 1)
            else:
                rises = lambda i: i // 2 + k < rings
                high = send(w, "seq", lambda i: i + 2 * k, rises)
            low = send(w, "seq", lambda i: i - 2 * k, lambda i: i // 2 >= k)
            table[("up", k, 0)] = (high, base)
            table[("down", k, 0)] = (low, base)
            risen = lambda i: i // 2 >= k
            fallen = lambda i: i // 2 < rings - k
            table[("up", k, 1)] = (send(high, "seq", swap, risen), base)
            table[("down", k, 1)] = (send(low, "seq", swap, fallen), base)
        tables.append(table)
    cache_pieces, query_pieces = tables

    scalars = (place1, block_doc, tail_len)
    pair = [("back", 0), ("pair", 0)]
    o_mine, o_theirs, *state = attend(
        scalars,
        [q_mine, q_near],
        [mine, near, above, across],
        [(parts, False)],
        pair + [("back", 2), ("pair", 2)],
        pair,
        SELF_TILE,
        "begin",
    )
    o_mine, o_theirs = attend(
        scalars,
        [q_mine, q_near],
        [far],
        [(parts, False)],
        [("odd", 2)],
        pair,
        SELF_TILE,
        "finish",
        [*state, o_mine, o_theirs],
    )
    both = lambda i: ((i // head) ^ 1) * head + ((i % head) ^ 2)
    route = [(i, both(i)) for i in range(seq * head)]
    corner = lax.ppermute(o_theirs, ("seq", "head"), route)
    flip = lambda i: i ^ 1
    places = jnp.stack([place, lane])
    contexts = [o_mine, send(o_theirs, "seq", swap), send(o_mine, "head", lambda i: i ^ 2), corner]
    others = [send(piece, "head", flip) for piece in contexts]
    partial = project_call(
        places,
        residual,
        contexts[:2] + others[:2],
        [w_blocks[0], w_blocks[2]],
        True,
        jnp.float32,
    )
    hidden = project_call(
        places,
        partial,
        contexts[2:] + others[2:],
        [w_blocks[1], w_blocks[3]],
        False,
        jnp.bfloat16,
    )
    hidden_x = send(hidden, "head", lambda i: i ^ 2)
    hidden_c = send(hidden, "head", lambda i: i ^ 1)
    hidden_xc = send(hidden_x, "head", lambda i: i ^ 1)
    normed, *caches = cache_call(
        place1,
        lane1,
        norm_gain[None, :],
        [hidden, hidden_c, hidden_x, hidden_xc],
        cache_pieces,
        wide,
        rings,
    )
    history = []
    for cache in caches:
        two = send(cache, "seq", up)
        chosen = jnp.where(side == 0, cache, two)
        one = send(chosen, "seq", swap)
        three = send(one, "seq", up)
        history.append([cache, two, one, three])
    cross_queries = query_call(place1, normed, query_pieces, wide, w_query.shape[1], rings)
    per = own // HEAD_DIM // groups
    shape = [(per, True)] * groups
    begun, *state = attend(
        scalars,
        [cross_queries],
        [slot for blocks in history for slot in blocks[:3]],
        shape,
        [("back", 0), ("back", 2), ("back", 1)],
        [("back", 0)],
        CROSS_TILE,
        "begin",
    )
    (cross_context,) = attend(
        scalars,
        [cross_queries],
        [blocks[3] for blocks in history],
        shape,
        [("back", 3)],
        [("back", 0)],
        CROSS_TILE,
        "finish",
        [*state, begun],
    )
    return (hidden, cross_context)


def direct_attend_kernel(
    place_ref, doc_ref, tail_ref, q_ref, *refs, slots, heads, group, q_tile, reach
):
    kv_refs = refs[: len(slots)]
    o_ref, m_ref, l_ref, acc_ref = refs[len(slots) :]
    rows = q_ref.shape[0]
    blocks = doc_ref.shape[0]
    kv_heads = heads // group
    factor = LOG2E / math.sqrt(HEAD_DIM)
    here = place_ref[0]
    own_doc = doc_ref[here]
    after = jnp.minimum(here + 1, blocks - 1)
    closing = jnp.logical_or(here == blocks - 1, doc_ref[after] != own_doc)
    live = jnp.where(closing, tail_ref[here], rows)

    def scores(kv_ref, t, h):
        q = q_ref[pl.ds(t, q_tile), h * HEAD_DIM : (h + 1) * HEAD_DIM]
        g = h // group
        k = kv_ref[:, g * HEAD_DIM : (g + 1) * HEAD_DIM]
        return lax.dot_general(q, k, (((1,), (1,)), ((), ())), preferred_element_type=jnp.float32)

    def values(kv_ref, h):
        g = kv_heads + h // group
        return kv_ref[:, g * HEAD_DIM : (g + 1) * HEAD_DIM]

    def tiles(step):
        def body(i, carry):
            step(pl.multiple_of(i * q_tile, q_tile))
            return carry

        lax.fori_loop(0, rows // q_tile, body, 0)

    def first(t):
        kv_ref = kv_refs[0]
        row = t + lax.broadcasted_iota(jnp.int32, (q_tile, rows), 0)
        col = lax.broadcasted_iota(jnp.int32, (q_tile, rows), 1)
        keep = jnp.logical_and(col <= row, col < live)
        for h in range(heads):
            s = jnp.where(keep, scores(kv_ref, t, h), -1e30)
            m = jnp.max(s, axis=1, keepdims=True)
            p = jnp.exp2((s - m) * factor)
            m_ref[h, pl.ds(t, q_tile), :] = jnp.broadcast_to(m, (q_tile, HEAD_DIM))
            l_ref[h, pl.ds(t, q_tile), :] = jnp.broadcast_to(
                jnp.sum(p, axis=1, keepdims=True), (q_tile, HEAD_DIM)
            )
            acc_ref[h, pl.ds(t, q_tile), :] = jnp.dot(
                p.astype(jnp.bfloat16), values(kv_ref, h), preferred_element_type=jnp.float32
            )

    def later(kv_ref, back):
        def step(t):
            if back * rows + rows - 1 >= reach:
                row = t + lax.broadcasted_iota(jnp.int32, (q_tile, rows), 0)
                col = lax.broadcasted_iota(jnp.int32, (q_tile, rows), 1)
                keep = back * rows + row - col < reach
            else:
                keep = None
            for h in range(heads):
                s = scores(kv_ref, t, h)
                if keep is not None:
                    s = jnp.where(keep, s, -1e30)
                m_old = m_ref[h, pl.ds(t, q_tile), :]
                m = jnp.maximum(m_old, jnp.max(s, axis=1, keepdims=True))
                shrink = jnp.exp2((m_old - m) * factor)
                p = jnp.exp2((s - m[:, :1]) * factor)
                m_ref[h, pl.ds(t, q_tile), :] = m
                l_ref[h, pl.ds(t, q_tile), :] = l_ref[h, pl.ds(t, q_tile), :] * shrink + jnp.sum(
                    p, axis=1, keepdims=True
                )
                acc_ref[h, pl.ds(t, q_tile), :] = acc_ref[
                    h, pl.ds(t, q_tile), :
                ] * shrink + jnp.dot(
                    p.astype(jnp.bfloat16), values(kv_ref, h), preferred_element_type=jnp.float32
                )

        return step

    tiles(first)
    for kv_ref, (even, odd) in zip(kv_refs[1:], slots[1:]):
        parity = lax.rem(here, 2)
        for back, only in ((even, 0), (odd, 1)):
            if back is None or (even == odd and only == 1):
                continue
            source = here - back
            wanted = jnp.logical_and(source >= 0, doc_ref[jnp.maximum(source, 0)] == own_doc)
            if even != odd:
                wanted = jnp.logical_and(wanted, parity == only)
            span = back

            @pl.when(wanted)
            def _(kv_ref=kv_ref, span=span):
                tiles(later(kv_ref, span))

    for h in range(heads):
        o_ref[:, h * HEAD_DIM : (h + 1) * HEAD_DIM] = (acc_ref[h] / l_ref[h]).astype(jnp.bfloat16)


def direct_attend(place, block_doc, tail_len, queries, column_block, heads, kv_list, slots, reach):
    rows, width = kv_list[0].shape
    kv_heads = width // (2 * HEAD_DIM)
    wide = heads * HEAD_DIM
    smem = pl.BlockSpec(memory_space=pltpu.SMEM)
    whole = pl.BlockSpec((rows, width), lambda i: (0, 0))
    return pl.pallas_call(
        functools.partial(
            direct_attend_kernel,
            slots=slots,
            heads=heads,
            group=heads // kv_heads,
            q_tile=min(256, rows),
            reach=reach,
        ),
        grid=(1,),
        out_shape=jax.ShapeDtypeStruct((rows, wide), jnp.bfloat16),
        in_specs=[smem, smem, smem, pl.BlockSpec((rows, wide), lambda i: (0, column_block))]
        + [whole] * len(kv_list),
        out_specs=pl.BlockSpec((rows, wide), lambda i: (0, 0)),
        scratch_shapes=[pltpu.VMEM((heads, rows, HEAD_DIM), jnp.float32)] * 3,
        compiler_params=pltpu.CompilerParams(vmem_limit_bytes=VMEM_LIMIT),
        name="attend",
    )(place, block_doc, tail_len, queries, *kv_list)


def direct_project_kernel(*refs, parts, blocks):
    residual_ref = refs[0]
    context_refs = refs[1 : 1 + parts * blocks]
    w_refs = refs[1 + parts * blocks : 1 + parts * blocks + blocks]
    o_ref = refs[-1]
    total = residual_ref[...].astype(jnp.float32)
    depth = context_refs[0].shape[1]
    for part in range(parts):
        for block in range(blocks):
            total += jnp.dot(
                context_refs[part * blocks + block][...],
                w_refs[block][part * depth : (part + 1) * depth, :],
                preferred_element_type=jnp.float32,
            )
    o_ref[...] = total.astype(jnp.bfloat16)


def norm_kernel(place_ref, gain_ref, *refs, near):
    hidden_refs, o_ref = refs[:-1], refs[-1]
    wide = hidden_refs[0].shape[1]
    total = 0.0
    for ref in hidden_refs:
        x = ref[...].astype(jnp.float32)
        total += jnp.sum(x * x, axis=1, keepdims=True)
    scale = lax.rsqrt(total / (wide * len(hidden_refs)) + EPSILON)
    for step, ref in enumerate(hidden_refs):
        at = pl.multiple_of(near(place_ref[0], step) * wide, wide)
        x = ref[...].astype(jnp.float32)
        o_ref[:, pl.ds(at, wide)] = (x * scale * gain_ref[:, pl.ds(at, wide)]).astype(jnp.bfloat16)


def columns_kernel(order_ref, normed_ref, *refs):
    w_refs, o_ref = refs[:-1], refs[-1]
    depth = w_refs[0].shape[0]
    total = 0.0
    for step, ref in enumerate(w_refs):
        at = pl.multiple_of(order_ref[step] * depth, depth)
        total += jnp.dot(
            normed_ref[:, pl.ds(at, depth)], ref[...], preferred_element_type=jnp.float32
        )
    o_ref[...] = total.astype(jnp.bfloat16)


def simple_call(kernel, out_shape, scalars, arrays):
    return pl.pallas_call(
        kernel,
        out_shape=out_shape,
        in_specs=[pl.BlockSpec(memory_space=pltpu.SMEM)] * len(scalars)
        + [pl.BlockSpec(memory_space=pltpu.VMEM)] * len(arrays),
        out_specs=pl.BlockSpec(memory_space=pltpu.VMEM),
        compiler_params=pltpu.CompilerParams(vmem_limit_bytes=VMEM_LIMIT),
    )(*scalars, *arrays)


def direct_layer(
    residual,
    q_self,
    k_self,
    v_self,
    w_out,
    norm_gain,
    w_query,
    w_cache,
    block_doc,
    tail_len,
    *,
    seq,
    head,
    span,
    paired,
):
    rows, own = residual.shape
    local_heads = q_self.shape[1] // HEAD_DIM
    place = lax.axis_index("seq").astype(jnp.int32)
    lane = lax.axis_index("head").astype(jnp.int32)
    place1, lane1 = place[None], lane[None]

    def along(block, target):
        return moved(block, "seq", seq, target)

    def across(block, step):
        return moved(block, "head", head, lambda i: i ^ step)

    even = lambda i: i % 2 == 0

    def spread(block):
        if not paired:
            return [along(block, lambda i, d=d: i + d) for d in range(1, span)]
        far = along(block, lambda i: i + 2)
        near = along(block, lambda i: i + 1 if even(i) else None)
        swap = along(far, lambda i: i ^ 1)
        last = along(swap, lambda i: i + 2 if even(i) else None)
        return [far, near, swap, last]

    if paired:
        slots = ((0, 0), (2, 2), (None, 1), (1, 3), (3, None))
    else:
        slots = tuple((d, d) for d in range(span))

    parts = local_heads // 2
    per = local_heads // parts
    width = per * HEAD_DIM
    kv_parts = []
    for c in range(parts):
        cols = slice(c * width, (c + 1) * width)
        own_kv = jnp.concatenate([k_self[:, cols], v_self[:, cols]], axis=1)
        kv_parts.append([own_kv] + spread(own_kv))

    w_blocks = []
    for step in range(head):
        piece = lax.dynamic_slice_in_dim(w_out, (lane ^ step) * own, own, 1)
        w_blocks.append(piece if step == 0 else across(piece, step))

    def gathered(w):
        if not paired:
            whole = lax.all_gather(w, "seq", axis=0, tiled=True)
            return [whole]
        pieces = [w, along(w, lambda i: i ^ 1)]
        ring = list(pieces)
        for distance in range(1, seq // 2):
            if distance <= seq // 4:
                ring = [along(p, lambda i: (i - 2) % seq) for p in ring]
                pieces += ring
            else:
                pieces += [
                    along(p, lambda i: (i + 2 * (seq // 2 - distance)) % seq) for p in pieces[:2]
                ]
        return pieces

    if paired:
        order = [(place ^ y) + 2 * distance for distance in range(seq // 2) for y in (0, 1)]
        order = jnp.stack([lax.rem(o, seq) for o in order])
    else:
        order = jnp.zeros((1,), jnp.int32)
    cache_w = gathered(w_cache)
    query_w = gathered(w_query)

    contexts = []
    for c in range(parts):
        mine = direct_attend(
            place1, block_doc, tail_len, q_self, c, per, kv_parts[c], slots, WINDOW
        )
        pair = [mine, across(mine, 2)]
        other = [across(p, 1) for p in pair]
        contexts += [pair[0], other[0], pair[1], other[1]]
    hidden = simple_call(
        functools.partial(direct_project_kernel, parts=parts, blocks=head),
        jax.ShapeDtypeStruct((rows, own), jnp.bfloat16),
        [],
        [residual, *contexts, *w_blocks],
    )
    pair = [hidden, across(hidden, 2)]
    other = [across(p, 1) for p in pair]
    normed = simple_call(
        functools.partial(norm_kernel, near=lambda at, step: at ^ step),
        jax.ShapeDtypeStruct((rows, own * head), jnp.bfloat16),
        [lane1],
        [norm_gain[None, :], pair[0], other[0], pair[1], other[1]],
    )
    cache = simple_call(
        columns_kernel,
        jax.ShapeDtypeStruct((rows, w_cache.shape[1]), jnp.bfloat16),
        [order],
        [normed, *cache_w],
    )
    history = [cache] + spread(cache)
    cross_queries = simple_call(
        columns_kernel,
        jax.ShapeDtypeStruct((rows, w_query.shape[1]), jnp.bfloat16),
        [order],
        [normed, *query_w],
    )
    cross_context = direct_attend(
        place1,
        block_doc,
        tail_len,
        cross_queries,
        0,
        local_heads,
        history,
        slots,
        rows * span,
    )
    return (hidden, cross_context)


def solution(mesh):
    seq, head = mesh.shape["seq"], mesh.shape["head"]
    span = min(5, seq // 2)
    in_specs = (
        P("seq", "head"),
        P("seq", "head"),
        P("seq", "head"),
        P("seq", "head"),
        P("head", None),
        P(),
        P("seq", "head"),
        P("seq", "head"),
        P(),
        P(),
    )
    out_specs = (P("seq", "head"), P("seq", "head"))
    if seq == 2 * span and head == 4:
        layer = functools.partial(paired_layer, seq=seq, head=head)
    else:
        layer = functools.partial(direct_layer, seq=seq, head=head, span=span, paired=False)

    def body(*args):
        return layer(*args)

    return jax.shard_map(body, mesh=mesh, in_specs=in_specs, out_specs=out_specs, check_vma=False)
```

```python
import functools
import math

import jax
import jax.numpy as jnp
from jax import lax
from jax.experimental import pallas as pl
from jax.experimental.pallas import tpu as pltpu
from jax.sharding import PartitionSpec as P


HEAD_DIM = 128
WINDOW = 2048
EPSILON = 1e-06
SELF_TILE = 256
VMEM_LIMIT = 24 * 2**20
PROJECT_LIMIT = 32 * 2**20
CROSS_TILE = 256
LOG2E = 1.4426950408889634


def moved(block, axis, size, target):
    route = [(i, target(i)) for i in range(size)]
    route = [(i, j) for i, j in route if j is not None and 0 <= j < size]
    return lax.ppermute(block, axis, route)


def attend_kernel(
    place_ref, doc_ref, tail_ref, *refs, arrays, groups, sources, q_sources, tile, mode
):
    count = len(sources) * len(groups)
    q_refs, refs = refs[:arrays], refs[arrays:]
    kv_refs, refs = refs[:count], refs[count:]
    if mode == "finish":
        ml_in, acc_in, *old_refs = refs[: 2 + arrays]
        o_refs = refs[2 + arrays :]
    else:
        o_refs, states = refs[:arrays], refs[arrays:]
    rows = q_refs[0].shape[0]
    blocks = doc_ref.shape[0]
    factor = LOG2E / math.sqrt(HEAD_DIM)
    here = place_ref[0]
    parity = lax.rem(here, 2)

    def lanes(at):
        if isinstance(at, int):
            return slice(at * HEAD_DIM, (at + 1) * HEAD_DIM)
        return pl.ds(pl.multiple_of(at * HEAD_DIM, HEAD_DIM), HEAD_DIM)

    def block_of(source):
        if source[0] == "back":
            return here - source[1]
        if source[0] == "pair":
            return here + 1 - 2 * parity - source[1]
        return here - parity - 1 - source[1]

    def joined(key_block, query_block):
        safe = jnp.maximum(key_block, 0)
        wanted = jnp.logical_and(key_block >= 0, key_block < query_block)
        return jnp.logical_and(wanted, doc_ref[safe] == doc_ref[query_block])

    def live_rows(block):
        after = jnp.minimum(block + 1, blocks - 1)
        closing = jnp.logical_or(block == blocks - 1, doc_ref[after] != doc_ref[block])
        return jnp.where(closing, tail_ref[block], rows)

    def soften(q, spans, before):
        k = jnp.concatenate([k for k, _, _, _ in spans], axis=0)
        v = jnp.concatenate([v for _, v, _, _ in spans], axis=0)
        v = jnp.concatenate([v, jnp.ones(v.shape, v.dtype)], axis=1)
        s_all = lax.dot_general(q, k, (((1,), (1,)), ((), ())), preferred_element_type=jnp.float32)
        parts, at = [], 0
        m = None if before is None else before[0]
        for k, _, keep, open_span in spans:
            s = s_all[:, at : at + k.shape[0]]
            at += k.shape[0]
            if keep is not None:
                s = jnp.where(keep, s, -1e30)
            peak = jnp.max(s, axis=1, keepdims=True)
            if open_span is not None:
                peak = jnp.where(open_span, peak, -1e30)
            m = peak if m is None else jnp.maximum(m, peak)
            parts.append((s, open_span))
        weights = []
        for s, open_span in parts:
            top = m if open_span is None else jnp.where(open_span, m, 1e30)
            weights.append(jnp.exp2((s - top) * factor).astype(jnp.bfloat16))
        acc = jnp.dot(
            jnp.concatenate(weights, axis=1), v, preferred_element_type=jnp.float32
        )
        if before is not None:
            shrink = jnp.exp2((before[0] - m) * factor)
            return m, acc[:, HEAD_DIM:] + before[1] * shrink, acc[:, :HEAD_DIM] + before[2] * shrink
        return m, acc[:, HEAD_DIM:], acc[:, :HEAD_DIM]

    def state_lane(index):
        return lax.broadcasted_iota(jnp.int32, (tile, HEAD_DIM), 1) == index

    def over_heads(body):
        for g, (heads, shared) in enumerate(groups):
            slots = kv_refs[g * len(sources) : (g + 1) * len(sources)]
            kv_heads = slots[0].shape[1] // (2 * HEAD_DIM)

            def one(h, carry, g=g, heads=heads, shared=shared, slots=slots, kv_heads=kv_heads):
                at = 0 if shared else h

                def pick(slot, keys):
                    return slot[:keys, lanes(at)], slot[:keys, lanes(kv_heads + at)]

                body(slots, g * heads + h, pick)
                return carry

            lax.fori_loop(0, heads, one, 0)

    def begin(slots, head, pick):
        def visit(n, extra):
            query_block = block_of(q_sources[n])
            live = live_rows(query_block)
            for t in range(0, rows, tile):
                keys = t + tile
                row = t + lax.broadcasted_iota(jnp.int32, (tile, keys), 0)
                col = lax.broadcasted_iota(jnp.int32, (tile, keys), 1)
                keep = jnp.logical_and(col <= row, col < live)
                spans = [(*pick(slots[sources.index(q_sources[n])], keys), keep, None)]
                for slot, source in zip(slots, sources):
                    if source not in q_sources or source == extra:
                        spans.append((*pick(slot, rows), None, joined(block_of(source), query_block)))
                m, total, acc = soften(q_refs[n][t : t + tile, lanes(head)], spans, None)
                o_refs[n][t : t + tile, lanes(head)] = (acc / total).astype(jnp.bfloat16)
                if arrays == 1 or extra is None:
                    ml_out, acc_out = states
                    acc_out[t : t + tile, lanes(head)] = acc
                    kept = jnp.where(state_lane(2 * head), m, ml_out[t : t + tile, :])
                    ml_out[t : t + tile, :] = jnp.where(state_lane(2 * head + 1), total, kept)

        if arrays == 1:
            visit(0, None)
            return
        for first in (0, 1):

            @pl.when(parity == first)
            def _(first=first):
                visit(first, None)
                visit(1 - first, q_sources[first])

    def finish(slots, head, pick):
        for n, (q_ref, old_ref, o_ref) in enumerate(zip(q_refs, old_refs, o_refs)):

            def go(q_ref=q_ref, o_ref=o_ref, n=n):
                query_block = block_of(q_sources[n])
                for t in range(0, rows, tile):
                    ml = ml_in[t : t + tile, :]
                    before = [
                        jnp.sum(jnp.where(state_lane(2 * head + i), ml, 0.0), axis=1, keepdims=True)
                        for i in (0, 1)
                    ]
                    before.append(acc_in[t : t + tile, lanes(head)])
                    spans = [
                        (*pick(slot, rows), None, joined(block_of(source), query_block))
                        for slot, source in zip(slots, sources)
                    ]
                    _, total, acc = soften(q_ref[t : t + tile, lanes(head)], spans, before)
                    o_ref[t : t + tile, lanes(head)] = (acc / total).astype(jnp.bfloat16)

            if arrays == 1:
                go()
            else:
                pl.when(parity == n)(go)

                @pl.when(parity != n)
                def _(old_ref=old_ref, o_ref=o_ref):
                    o_ref[:, lanes(head)] = old_ref[:, lanes(head)]

    if mode == "begin":
        states[0][...] = jnp.zeros(states[0].shape, jnp.float32)
    over_heads(finish if mode == "finish" else begin)


def attend(scalars, q_list, kv_list, groups, sources, q_sources, tile, mode, state=()):
    rows, wide = q_list[0].shape
    arrays = len(q_list)
    smem = pl.BlockSpec(memory_space=pltpu.SMEM)
    vmem = pl.BlockSpec(memory_space=pltpu.VMEM)
    heads = sum(g[0] for g in groups)
    operands = [*q_list, *kv_list, *state]
    out_shape = [jax.ShapeDtypeStruct((rows, wide), jnp.bfloat16)] * arrays
    if mode == "begin":
        out_shape += [
            jax.ShapeDtypeStruct((rows, d * HEAD_DIM), jnp.float32) for d in (1, heads)
        ]
    return pl.pallas_call(
        functools.partial(
            attend_kernel,
            arrays=arrays,
            groups=tuple(groups),
            sources=tuple(sources),
            q_sources=tuple(q_sources),
            tile=min(tile, rows),
            mode=mode,
        ),
        out_shape=out_shape,
        in_specs=[smem] * len(scalars) + [vmem] * len(operands),
        out_specs=[vmem] * len(out_shape),
        compiler_params=pltpu.CompilerParams(vmem_limit_bytes=VMEM_LIMIT),
        name="attend",
    )(*scalars, *operands)


def project_call(places, base, pieces, w_blocks, first, out_type):
    rows, own = base.shape
    half = own // 2

    def kernel(places_ref, base_ref, *refs):
        near_refs, w_refs = refs[: len(pieces)], refs[len(pieces) : -2]
        o_ref, context_ref = refs[-2:]
        side = lax.rem(places_ref[0], 2)
        for step, ref in enumerate(near_refs):
            block, other = divmod(step, 2)
            at = block * own + (side if other == 0 else 1 - side) * half
            context_ref[:, pl.ds(pl.multiple_of(at, half), half)] = ref[...]
        total = base_ref[...].astype(jnp.float32)
        for block, w_ref in enumerate(w_refs):
            total += jnp.dot(
                context_ref[:, block * own : (block + 1) * own],
                w_ref[...],
                preferred_element_type=jnp.float32,
            )
        o_ref[...] = total.astype(o_ref.dtype)

    whole = lambda a: pl.BlockSpec(a.shape, lambda i, places_ref: (0, 0))
    corner = pl.BlockSpec((own, own), lambda i, places_ref: (0, places_ref[1] if first else 0))
    return pl.pallas_call(
        kernel,
        grid_spec=pltpu.PrefetchScalarGridSpec(
            num_scalar_prefetch=1,
            grid=(1,),
            in_specs=[whole(a) for a in (base, *pieces)]
            + [corner]
            + [whole(w) for w in w_blocks[1:]],
            out_specs=whole(base),
            scratch_shapes=[pltpu.VMEM((rows, own * len(w_blocks)), jnp.bfloat16)],
        ),
        out_shape=jax.ShapeDtypeStruct((rows, own), out_type),
        compiler_params=pltpu.CompilerParams(vmem_limit_bytes=VMEM_LIMIT),
        name="project",
    )(places, base, *pieces, *w_blocks)


def norm_into(lane, gain_ref, pieces, at_row, normed_ref):
    wide = pieces[0][0].shape[1]
    rows = pieces[0][1].stop - pieces[0][1].start
    total = 0.0
    for ref, part in pieces:
        x = ref[part, :].astype(jnp.float32)
        total += jnp.sum(x * x, axis=1, keepdims=True)
    scale = lax.rsqrt(total / (wide * len(pieces)) + EPSILON)
    for step, (ref, part) in enumerate(pieces):
        at = pl.multiple_of((lane ^ step) * wide, wide)
        x = ref[part, :].astype(jnp.float32)
        normed_ref[at_row : at_row + rows, pl.ds(at, wide)] = (
            x * scale * gain_ref[:, pl.ds(at, wide)]
        ).astype(jnp.bfloat16)


def fetch(place_ref, pieces, buffer, sems, rings):
    z = place_ref[0] // 2
    for k in range(rings):

        def begin(name, k=k):
            pltpu.make_async_copy(pieces[name], buffer.at[k], sems.at[k]).start()

        if k == 0:
            begin(("w", 0))
        else:

            @pl.when(z >= k)
            def _(k=k, begin=begin):
                begin(("up", k))

            @pl.when(z < k)
            def _(k=k, begin=begin):
                begin(("down", rings - k))


def gather_dot(place_ref, normed, pieces, buffer, sems, rings):
    z = place_ref[0] // 2
    depth = buffer.shape[1]
    total = 0.0
    for k in range(rings):
        if sems is not None:
            pltpu.make_async_copy(pieces[("w", 0)], buffer.at[k], sems.at[k]).wait()
        at = pl.multiple_of(lax.rem(z - k + rings, rings) * depth, depth)
        total += jnp.dot(normed[:, pl.ds(at, depth)], buffer[k], preferred_element_type=jnp.float32)
    return total


def cache_call(place1, lane1, gain, hiddens, pieces, rings):
    names = list(pieces)
    depth, width = pieces[("w", 0)].shape
    arrays = [a for _, group in hiddens for a, _ in group]
    total = sum(part.stop - part.start for _, ((_, part), *_) in hiddens)
    wide = arrays[0].shape[1] * len(hiddens[0][1])

    def kernel(place_ref, lane_ref, gain_ref, *refs):
        hidden_refs = refs[: len(arrays)]
        piece_refs = refs[len(arrays) : len(arrays) + len(names)]
        normed_ref, cache_ref, buffer, sems = refs[len(arrays) + len(names) :]
        at = dict(zip(names, piece_refs))
        fetch(place_ref, at, buffer, sems, rings)
        taken = 0
        for row, group in hiddens:
            pairs = [(hidden_refs[taken + n], part) for n, (_, part) in enumerate(group)]
            taken += len(group)
            norm_into(lane_ref[0], gain_ref, pairs, row, normed_ref)
        cache_ref[...] = gather_dot(place_ref, normed_ref, at, buffer, sems, rings).astype(
            jnp.bfloat16
        )

    vmem = pl.BlockSpec(memory_space=pltpu.VMEM)
    smem = pl.BlockSpec(memory_space=pltpu.SMEM)
    return pl.pallas_call(
        kernel,
        out_shape=[
            jax.ShapeDtypeStruct((total, wide), jnp.bfloat16),
            jax.ShapeDtypeStruct((total, width), jnp.bfloat16),
        ],
        in_specs=[smem, smem, vmem]
        + [vmem] * len(arrays)
        + [pl.BlockSpec(memory_space=pl.ANY)] * len(names),
        out_specs=[vmem] * 2,
        scratch_shapes=[
            pltpu.VMEM((rings, depth, width), jnp.bfloat16),
            pltpu.SemaphoreType.DMA((rings,)),
        ],
        compiler_params=pltpu.CompilerParams(vmem_limit_bytes=PROJECT_LIMIT),
        name="cache",
    )(place1, lane1, gain, *arrays, *[pieces[n] for n in names])


def query_call(place1, normed, pieces, rings):
    names = list(pieces)
    depth, width = pieces[("w", 0)].shape
    count = len(normed)

    def kernel(place_ref, *refs):
        normed_refs, refs = refs[:count], refs[count:]
        piece_refs, refs = refs[: len(names)], refs[len(names) :]
        o_refs, (buffer, sems) = refs[:count], refs[count:]
        at = dict(zip(names, piece_refs))
        fetch(place_ref, at, buffer, sems, rings)
        for n in range(count):
            o_refs[n][...] = gather_dot(
                place_ref, normed_refs[n], at, buffer, None if n else sems, rings
            ).astype(jnp.bfloat16)

    vmem = pl.BlockSpec(memory_space=pltpu.VMEM)
    return pl.pallas_call(
        kernel,
        out_shape=[jax.ShapeDtypeStruct((a.shape[0], width), jnp.bfloat16) for a in normed],
        in_specs=[pl.BlockSpec(memory_space=pltpu.SMEM)]
        + [vmem] * count
        + [pl.BlockSpec(memory_space=pl.ANY)] * len(names),
        out_specs=[vmem] * count,
        scratch_shapes=[
            pltpu.VMEM((rings, depth, width), jnp.bfloat16),
            pltpu.SemaphoreType.DMA((rings,)),
        ],
        compiler_params=pltpu.CompilerParams(vmem_limit_bytes=PROJECT_LIMIT),
        name="queries",
    )(place1, *normed, *[pieces[n] for n in names])


def paired_layer(
    residual,
    q_self,
    k_self,
    v_self,
    w_out,
    norm_gain,
    w_query,
    w_cache,
    block_doc,
    tail_len,
    *,
    seq,
    head,
):
    rows, own = residual.shape
    half = own // 2
    parts = half // HEAD_DIM
    rings = seq // 2
    place = lax.axis_index("seq").astype(jnp.int32)
    lane = lax.axis_index("head").astype(jnp.int32)
    side = lax.rem(place, 2)
    place1, lane1 = place[None], lane[None]

    def send(block, axis, target, source=None):
        size = seq if axis == "seq" else head
        return moved(
            block, axis, size, lambda i: target(i) if source is None or source(i) else None
        )

    up = lambda i: i + 2
    down = lambda i: i - 2
    swap = lambda i: i ^ 1
    column = lambda a, at, size: lax.dynamic_slice_in_dim(a, at, size, 1)

    def kv_of(which):
        at = which * half
        return jnp.concatenate([column(k_self, at, half), column(v_self, at, half)], axis=1)

    mine, theirs = kv_of(side), kv_of(1 - side)
    q_mine = column(q_self, side * half, half)
    q_theirs = column(q_self, (1 - side) * half, half)
    above = send(mine, "seq", up)
    near = send(theirs, "seq", swap)
    across = send(near, "seq", up)
    odd = jnp.where(side == 1, above, across)
    far = send(odd, "seq", up, lambda i: i >= 2)
    q_near = send(q_theirs, "seq", swap)

    w_blocks = [w_out]
    late = lax.optimization_barrier(w_out)
    for step in (2, 1, 3):
        source = late if step == 1 else w_out
        piece = lax.dynamic_slice_in_dim(source, (lane ^ step) * own, own, 1)
        w_blocks.append(send(piece, "head", lambda i: i ^ step))

    kv_width = w_cache.shape[1] // 2
    kv_half = kv_width // 2

    def columns_of(which):
        return jnp.concatenate(
            [
                column(w_cache, which * kv_half, kv_half),
                column(w_cache, kv_width + which * kv_half, kv_half),
                column(w_query, which * half, half),
            ],
            axis=1,
        )

    def ordered(kept, got, axis):
        return jnp.where(
            side == 0,
            jnp.concatenate([kept, got], axis=axis),
            jnp.concatenate([got, kept], axis=axis),
        )

    w_kept = columns_of(side)
    w_got = send(columns_of(1 - side), "seq", swap)
    tables = []
    for start, stop in ((0, kv_width), (kv_width, kv_width + half)):
        w = ordered(w_kept[:, start:stop], w_got[:, start:stop], 0)
        table = {("w", 0): w}
        high = low = w
        for k in range(1, rings):
            high = send(high, "seq", up, lambda i: i // 2 >= k - 1)
            low = send(low, "seq", down, lambda i: i // 2 <= rings - k)
            table[("up", k)] = high
            table[("down", k)] = low
        tables.append(table)
    cache_pieces, query_pieces = tables

    scalars = (place1, block_doc, tail_len)
    pair = [("back", 0), ("pair", 0)]
    o_mine, o_theirs, *state = attend(
        scalars,
        [q_mine, q_near],
        [mine, near, above, across],
        [(parts, False)],
        pair + [("back", 2), ("pair", 2)],
        pair,
        SELF_TILE,
        "begin",
    )
    o_mine, o_theirs = attend(
        scalars,
        [q_mine, q_near],
        [far],
        [(parts, False)],
        [("odd", 2)],
        pair,
        SELF_TILE,
        "finish",
        [*state, o_mine, o_theirs],
    )
    both = lambda i: ((i // head) ^ 1) * head + ((i % head) ^ 2)
    route = [(i, both(i)) for i in range(seq * head)]
    corner = lax.ppermute(o_theirs, ("seq", "head"), route)
    flip = lambda i: i ^ 1
    places = jnp.stack([place, lane])
    contexts = [o_mine, send(o_theirs, "seq", swap), send(o_mine, "head", lambda i: i ^ 2), corner]
    others = [send(piece, "head", flip) for piece in contexts]
    partial = project_call(
        places,
        residual,
        contexts[:2] + others[:2],
        [w_blocks[0], w_blocks[2]],
        True,
        jnp.float32,
    )
    hidden = project_call(
        places,
        partial,
        contexts[2:] + others[2:],
        [w_blocks[1], w_blocks[3]],
        False,
        jnp.bfloat16,
    )
    cut = rows // 2
    beside = lambda i: i ^ 2
    hidden_x = send(hidden, "head", beside)
    hidden_y = send(hidden, "seq", swap)
    corner_a = send(hidden_x[:cut], "seq", swap)
    corner_b = send(hidden_y[cut:], "head", beside)
    core = {}
    for name, piece in (
        ("hc", hidden),
        ("hxc", hidden_x),
        ("hyc", hidden_y),
        ("hxyac", corner_a),
        ("hxybc", corner_b),
    ):
        core[name] = send(piece, "head", flip)
    every, low_rows, high_rows = slice(0, rows), slice(0, cut), slice(cut, rows)
    gain = norm_gain[None, :]
    group = [(0, [(a, every) for a in (hidden, core["hc"], hidden_x, core["hxc"])])]
    normed_mine, cache_mine = cache_call(place1, lane1, gain, group, cache_pieces, rings)
    groups = [
        (
            0,
            [(hidden_y, low_rows), (core["hyc"], low_rows)]
            + [(a, low_rows) for a in (corner_a, core["hxyac"])],
        ),
        (
            cut,
            [(hidden_y, high_rows), (core["hyc"], high_rows)]
            + [(a, low_rows) for a in (corner_b, core["hxybc"])],
        ),
    ]
    normed_near, cache_near = cache_call(place1, lane1, gain, groups, cache_pieces, rings)
    q_pair = query_call(place1, [normed_mine, normed_near], query_pieces, rings)
    cache_above = send(cache_mine, "seq", up)
    cache_across = send(cache_near, "seq", up)
    cache_odd = jnp.where(side == 1, cache_above, cache_across)
    cache_far = send(cache_odd, "seq", up, lambda i: i >= 2)
    o_mine, o_theirs, *state = attend(
        scalars,
        q_pair,
        [cache_mine, cache_near, cache_above, cache_across],
        [(parts, True)],
        pair + [("back", 2), ("pair", 2)],
        pair,
        CROSS_TILE,
        "begin",
    )
    o_mine, o_theirs = attend(
        scalars,
        q_pair,
        [cache_far],
        [(parts, True)],
        [("odd", 2)],
        pair,
        CROSS_TILE,
        "finish",
        [*state, o_mine, o_theirs],
    )
    cross_context = ordered(o_mine, send(o_theirs, "seq", swap), 1)
    return (hidden, cross_context)


def direct_attend_kernel(
    place_ref, doc_ref, tail_ref, q_ref, *refs, slots, heads, group, q_tile, reach
):
    kv_refs = refs[: len(slots)]
    o_ref, m_ref, l_ref, acc_ref = refs[len(slots) :]
    rows = q_ref.shape[0]
    blocks = doc_ref.shape[0]
    kv_heads = heads // group
    factor = LOG2E / math.sqrt(HEAD_DIM)
    here = place_ref[0]
    own_doc = doc_ref[here]
    after = jnp.minimum(here + 1, blocks - 1)
    closing = jnp.logical_or(here == blocks - 1, doc_ref[after] != own_doc)
    live = jnp.where(closing, tail_ref[here], rows)

    def scores(kv_ref, t, h):
        q = q_ref[pl.ds(t, q_tile), h * HEAD_DIM : (h + 1) * HEAD_DIM]
        g = h // group
        k = kv_ref[:, g * HEAD_DIM : (g + 1) * HEAD_DIM]
        return lax.dot_general(q, k, (((1,), (1,)), ((), ())), preferred_element_type=jnp.float32)

    def values(kv_ref, h):
        g = kv_heads + h // group
        return kv_ref[:, g * HEAD_DIM : (g + 1) * HEAD_DIM]

    def tiles(step):
        def body(i, carry):
            step(pl.multiple_of(i * q_tile, q_tile))
            return carry

        lax.fori_loop(0, rows // q_tile, body, 0)

    def first(t):
        kv_ref = kv_refs[0]
        row = t + lax.broadcasted_iota(jnp.int32, (q_tile, rows), 0)
        col = lax.broadcasted_iota(jnp.int32, (q_tile, rows), 1)
        keep = jnp.logical_and(col <= row, col < live)
        for h in range(heads):
            s = jnp.where(keep, scores(kv_ref, t, h), -1e30)
            m = jnp.max(s, axis=1, keepdims=True)
            p = jnp.exp2((s - m) * factor)
            m_ref[h, pl.ds(t, q_tile), :] = jnp.broadcast_to(m, (q_tile, HEAD_DIM))
            l_ref[h, pl.ds(t, q_tile), :] = jnp.broadcast_to(
                jnp.sum(p, axis=1, keepdims=True), (q_tile, HEAD_DIM)
            )
            acc_ref[h, pl.ds(t, q_tile), :] = jnp.dot(
                p.astype(jnp.bfloat16), values(kv_ref, h), preferred_element_type=jnp.float32
            )

    def later(kv_ref, back):
        def step(t):
            if back * rows + rows - 1 >= reach:
                row = t + lax.broadcasted_iota(jnp.int32, (q_tile, rows), 0)
                col = lax.broadcasted_iota(jnp.int32, (q_tile, rows), 1)
                keep = back * rows + row - col < reach
            else:
                keep = None
            for h in range(heads):
                s = scores(kv_ref, t, h)
                if keep is not None:
                    s = jnp.where(keep, s, -1e30)
                m_old = m_ref[h, pl.ds(t, q_tile), :]
                m = jnp.maximum(m_old, jnp.max(s, axis=1, keepdims=True))
                shrink = jnp.exp2((m_old - m) * factor)
                p = jnp.exp2((s - m[:, :1]) * factor)
                m_ref[h, pl.ds(t, q_tile), :] = m
                l_ref[h, pl.ds(t, q_tile), :] = l_ref[h, pl.ds(t, q_tile), :] * shrink + jnp.sum(
                    p, axis=1, keepdims=True
                )
                acc_ref[h, pl.ds(t, q_tile), :] = acc_ref[
                    h, pl.ds(t, q_tile), :
                ] * shrink + jnp.dot(
                    p.astype(jnp.bfloat16), values(kv_ref, h), preferred_element_type=jnp.float32
                )

        return step

    tiles(first)
    for kv_ref, (even, odd) in zip(kv_refs[1:], slots[1:]):
        parity = lax.rem(here, 2)
        for back, only in ((even, 0), (odd, 1)):
            if back is None or (even == odd and only == 1):
                continue
            source = here - back
            wanted = jnp.logical_and(source >= 0, doc_ref[jnp.maximum(source, 0)] == own_doc)
            if even != odd:
                wanted = jnp.logical_and(wanted, parity == only)
            span = back

            @pl.when(wanted)
            def _(kv_ref=kv_ref, span=span):
                tiles(later(kv_ref, span))

    for h in range(heads):
        o_ref[:, h * HEAD_DIM : (h + 1) * HEAD_DIM] = (acc_ref[h] / l_ref[h]).astype(jnp.bfloat16)


def direct_attend(place, block_doc, tail_len, queries, column_block, heads, kv_list, slots, reach):
    rows, width = kv_list[0].shape
    kv_heads = width // (2 * HEAD_DIM)
    wide = heads * HEAD_DIM
    smem = pl.BlockSpec(memory_space=pltpu.SMEM)
    whole = pl.BlockSpec((rows, width), lambda i: (0, 0))
    return pl.pallas_call(
        functools.partial(
            direct_attend_kernel,
            slots=slots,
            heads=heads,
            group=heads // kv_heads,
            q_tile=min(256, rows),
            reach=reach,
        ),
        grid=(1,),
        out_shape=jax.ShapeDtypeStruct((rows, wide), jnp.bfloat16),
        in_specs=[smem, smem, smem, pl.BlockSpec((rows, wide), lambda i: (0, column_block))]
        + [whole] * len(kv_list),
        out_specs=pl.BlockSpec((rows, wide), lambda i: (0, 0)),
        scratch_shapes=[pltpu.VMEM((heads, rows, HEAD_DIM), jnp.float32)] * 3,
        compiler_params=pltpu.CompilerParams(vmem_limit_bytes=VMEM_LIMIT),
        name="attend",
    )(place, block_doc, tail_len, queries, *kv_list)


def direct_project_kernel(*refs, parts, blocks):
    residual_ref = refs[0]
    context_refs = refs[1 : 1 + parts * blocks]
    w_refs = refs[1 + parts * blocks : 1 + parts * blocks + blocks]
    o_ref = refs[-1]
    total = residual_ref[...].astype(jnp.float32)
    depth = context_refs[0].shape[1]
    for part in range(parts):
        for block in range(blocks):
            total += jnp.dot(
                context_refs[part * blocks + block][...],
                w_refs[block][part * depth : (part + 1) * depth, :],
                preferred_element_type=jnp.float32,
            )
    o_ref[...] = total.astype(jnp.bfloat16)


def norm_kernel(place_ref, gain_ref, *refs, near):
    hidden_refs, o_ref = refs[:-1], refs[-1]
    wide = hidden_refs[0].shape[1]
    total = 0.0
    for ref in hidden_refs:
        x = ref[...].astype(jnp.float32)
        total += jnp.sum(x * x, axis=1, keepdims=True)
    scale = lax.rsqrt(total / (wide * len(hidden_refs)) + EPSILON)
    for step, ref in enumerate(hidden_refs):
        at = pl.multiple_of(near(place_ref[0], step) * wide, wide)
        x = ref[...].astype(jnp.float32)
        o_ref[:, pl.ds(at, wide)] = (x * scale * gain_ref[:, pl.ds(at, wide)]).astype(jnp.bfloat16)


def columns_kernel(order_ref, normed_ref, *refs):
    w_refs, o_ref = refs[:-1], refs[-1]
    depth = w_refs[0].shape[0]
    total = 0.0
    for step, ref in enumerate(w_refs):
        at = pl.multiple_of(order_ref[step] * depth, depth)
        total += jnp.dot(
            normed_ref[:, pl.ds(at, depth)], ref[...], preferred_element_type=jnp.float32
        )
    o_ref[...] = total.astype(jnp.bfloat16)


def simple_call(kernel, out_shape, scalars, arrays):
    return pl.pallas_call(
        kernel,
        out_shape=out_shape,
        in_specs=[pl.BlockSpec(memory_space=pltpu.SMEM)] * len(scalars)
        + [pl.BlockSpec(memory_space=pltpu.VMEM)] * len(arrays),
        out_specs=pl.BlockSpec(memory_space=pltpu.VMEM),
        compiler_params=pltpu.CompilerParams(vmem_limit_bytes=VMEM_LIMIT),
    )(*scalars, *arrays)


def direct_layer(
    residual,
    q_self,
    k_self,
    v_self,
    w_out,
    norm_gain,
    w_query,
    w_cache,
    block_doc,
    tail_len,
    *,
    seq,
    head,
    span,
    paired,
):
    rows, own = residual.shape
    local_heads = q_self.shape[1] // HEAD_DIM
    place = lax.axis_index("seq").astype(jnp.int32)
    lane = lax.axis_index("head").astype(jnp.int32)
    place1, lane1 = place[None], lane[None]

    def along(block, target):
        return moved(block, "seq", seq, target)

    def across(block, step):
        return moved(block, "head", head, lambda i: i ^ step)

    even = lambda i: i % 2 == 0

    def spread(block):
        if not paired:
            return [along(block, lambda i, d=d: i + d) for d in range(1, span)]
        far = along(block, lambda i: i + 2)
        near = along(block, lambda i: i + 1 if even(i) else None)
        swap = along(far, lambda i: i ^ 1)
        last = along(swap, lambda i: i + 2 if even(i) else None)
        return [far, near, swap, last]

    if paired:
        slots = ((0, 0), (2, 2), (None, 1), (1, 3), (3, None))
    else:
        slots = tuple((d, d) for d in range(span))

    parts = local_heads // 2
    per = local_heads // parts
    width = per * HEAD_DIM
    kv_parts = []
    for c in range(parts):
        cols = slice(c * width, (c + 1) * width)
        own_kv = jnp.concatenate([k_self[:, cols], v_self[:, cols]], axis=1)
        kv_parts.append([own_kv] + spread(own_kv))

    w_blocks = []
    for step in range(head):
        piece = lax.dynamic_slice_in_dim(w_out, (lane ^ step) * own, own, 1)
        w_blocks.append(piece if step == 0 else across(piece, step))

    def gathered(w):
        if not paired:
            whole = lax.all_gather(w, "seq", axis=0, tiled=True)
            return [whole]
        pieces = [w, along(w, lambda i: i ^ 1)]
        ring = list(pieces)
        for distance in range(1, seq // 2):
            if distance <= seq // 4:
                ring = [along(p, lambda i: (i - 2) % seq) for p in ring]
                pieces += ring
            else:
                pieces += [
                    along(p, lambda i: (i + 2 * (seq // 2 - distance)) % seq) for p in pieces[:2]
                ]
        return pieces

    if paired:
        order = [(place ^ y) + 2 * distance for distance in range(seq // 2) for y in (0, 1)]
        order = jnp.stack([lax.rem(o, seq) for o in order])
    else:
        order = jnp.zeros((1,), jnp.int32)
    cache_w = gathered(w_cache)
    query_w = gathered(w_query)

    contexts = []
    for c in range(parts):
        mine = direct_attend(
            place1, block_doc, tail_len, q_self, c, per, kv_parts[c], slots, WINDOW
        )
        pair = [mine, across(mine, 2)]
        other = [across(p, 1) for p in pair]
        contexts += [pair[0], other[0], pair[1], other[1]]
    hidden = simple_call(
        functools.partial(direct_project_kernel, parts=parts, blocks=head),
        jax.ShapeDtypeStruct((rows, own), jnp.bfloat16),
        [],
        [residual, *contexts, *w_blocks],
    )
    pair = [hidden, across(hidden, 2)]
    other = [across(p, 1) for p in pair]
    normed = simple_call(
        functools.partial(norm_kernel, near=lambda at, step: at ^ step),
        jax.ShapeDtypeStruct((rows, own * head), jnp.bfloat16),
        [lane1],
        [norm_gain[None, :], pair[0], other[0], pair[1], other[1]],
    )
    cache = simple_call(
        columns_kernel,
        jax.ShapeDtypeStruct((rows, w_cache.shape[1]), jnp.bfloat16),
        [order],
        [normed, *cache_w],
    )
    history = [cache] + spread(cache)
    cross_queries = simple_call(
        columns_kernel,
        jax.ShapeDtypeStruct((rows, w_query.shape[1]), jnp.bfloat16),
        [order],
        [normed, *query_w],
    )
    cross_context = direct_attend(
        place1,
        block_doc,
        tail_len,
        cross_queries,
        0,
        local_heads,
        history,
        slots,
        rows * span,
    )
    return (hidden, cross_context)


def solution(mesh):
    seq, head = mesh.shape["seq"], mesh.shape["head"]
    span = min(5, seq // 2)
    in_specs = (
        P("seq", "head"),
        P("seq", "head"),
        P("seq", "head"),
        P("seq", "head"),
        P("head", None),
        P(),
        P("seq", "head"),
        P("seq", "head"),
        P(),
        P(),
    )
    out_specs = (P("seq", "head"), P("seq", "head"))
    if seq == 2 * span and head == 4:
        layer = functools.partial(paired_layer, seq=seq, head=head)
    else:
        layer = functools.partial(direct_layer, seq=seq, head=head, span=span, paired=False)

    def body(*args):
        return layer(*args)

    return jax.shard_map(body, mesh=mesh, in_specs=in_specs, out_specs=out_specs, check_vma=False)
```

```python
import functools
import math

import jax
import jax.numpy as jnp
from jax import lax
from jax.experimental import pallas as pl
from jax.experimental.pallas import tpu as pltpu
from jax.sharding import PartitionSpec as P


HEAD_DIM = 128
WINDOW = 2048
EPSILON = 1e-06
SELF_TILE = 256
VMEM_LIMIT = 24 * 2**20
PROJECT_LIMIT = 32 * 2**20
CROSS_TILE = 256
LOG2E = 1.4426950408889634


def moved(block, axis, size, target):
    route = [(i, target(i)) for i in range(size)]
    route = [(i, j) for i, j in route if j is not None and 0 <= j < size]
    return lax.ppermute(block, axis, route)


def attend_kernel(
    place_ref, doc_ref, tail_ref, *refs, arrays, groups, sources, q_sources, tile, mode
):
    count = len(sources) * len(groups)
    q_refs, refs = refs[:arrays], refs[arrays:]
    kv_refs, refs = refs[:count], refs[count:]
    if mode == "finish":
        ml_in, acc_in, *old_refs = refs[: 2 + arrays]
        o_refs = refs[2 + arrays :]
    else:
        o_refs, states = refs[:arrays], refs[arrays:]
    rows = q_refs[0].shape[0]
    blocks = doc_ref.shape[0]
    factor = LOG2E / math.sqrt(HEAD_DIM)
    here = place_ref[0]
    parity = lax.rem(here, 2)

    def lanes(at):
        if isinstance(at, int):
            return slice(at * HEAD_DIM, (at + 1) * HEAD_DIM)
        return pl.ds(pl.multiple_of(at * HEAD_DIM, HEAD_DIM), HEAD_DIM)

    def block_of(source):
        if source[0] == "back":
            return here - source[1]
        if source[0] == "pair":
            return here + 1 - 2 * parity - source[1]
        return here - parity - 1 - source[1]

    def joined(key_block, query_block):
        safe = jnp.maximum(key_block, 0)
        wanted = jnp.logical_and(key_block >= 0, key_block < query_block)
        return jnp.logical_and(wanted, doc_ref[safe] == doc_ref[query_block])

    def live_rows(block):
        after = jnp.minimum(block + 1, blocks - 1)
        closing = jnp.logical_or(block == blocks - 1, doc_ref[after] != doc_ref[block])
        return jnp.where(closing, tail_ref[block], rows)

    def soften(q, spans, before):
        k = jnp.concatenate([k for k, _, _, _ in spans], axis=0)
        v = jnp.concatenate([v for _, v, _, _ in spans], axis=0)
        v = jnp.concatenate([v, jnp.ones(v.shape, v.dtype)], axis=1)
        s_all = lax.dot_general(q, k, (((1,), (1,)), ((), ())), preferred_element_type=jnp.float32)
        parts, at = [], 0
        m = None if before is None else before[0]
        for k, _, keep, open_span in spans:
            s = s_all[:, at : at + k.shape[0]]
            at += k.shape[0]
            if keep is not None:
                s = jnp.where(keep, s, -1e30)
            peak = jnp.max(s, axis=1, keepdims=True)
            if open_span is not None:
                peak = jnp.where(open_span, peak, -1e30)
            m = peak if m is None else jnp.maximum(m, peak)
            parts.append((s, open_span))
        weights = []
        for s, open_span in parts:
            top = m if open_span is None else jnp.where(open_span, m, 1e30)
            weights.append(jnp.exp2((s - top) * factor).astype(jnp.bfloat16))
        acc = jnp.dot(
            jnp.concatenate(weights, axis=1), v, preferred_element_type=jnp.float32
        )
        if before is not None:
            shrink = jnp.exp2((before[0] - m) * factor)
            return m, acc[:, HEAD_DIM:] + before[1] * shrink, acc[:, :HEAD_DIM] + before[2] * shrink
        return m, acc[:, HEAD_DIM:], acc[:, :HEAD_DIM]

    def state_lane(index):
        return lax.broadcasted_iota(jnp.int32, (tile, HEAD_DIM), 1) == index

    def over_heads(body):
        for g, (heads, shared) in enumerate(groups):
            slots = kv_refs[g * len(sources) : (g + 1) * len(sources)]
            kv_heads = slots[0].shape[1] // (2 * HEAD_DIM)

            def one(h, carry, g=g, heads=heads, shared=shared, slots=slots, kv_heads=kv_heads):
                at = 0 if shared else h

                def pick(slot, keys):
                    return slot[:keys, lanes(at)], slot[:keys, lanes(kv_heads + at)]

                body(slots, g * heads + h, pick)
                return carry

            lax.fori_loop(0, heads, one, 0)

    def begin(slots, head, pick):
        def visit(n, extra):
            query_block = block_of(q_sources[n])
            live = live_rows(query_block)
            for t in range(0, rows, tile):
                keys = t + tile
                row = t + lax.broadcasted_iota(jnp.int32, (tile, keys), 0)
                col = lax.broadcasted_iota(jnp.int32, (tile, keys), 1)
                keep = jnp.logical_and(col <= row, col < live)
                spans = [(*pick(slots[sources.index(q_sources[n])], keys), keep, None)]
                for slot, source in zip(slots, sources):
                    if source not in q_sources or source == extra:
                        spans.append((*pick(slot, rows), None, joined(block_of(source), query_block)))
                m, total, acc = soften(q_refs[n][t : t + tile, lanes(head)], spans, None)
                o_refs[n][t : t + tile, lanes(head)] = (acc / total).astype(jnp.bfloat16)
                if arrays == 1 or extra is None:
                    ml_out, acc_out = states
                    acc_out[t : t + tile, lanes(head)] = acc
                    kept = jnp.where(state_lane(2 * head), m, ml_out[t : t + tile, :])
                    ml_out[t : t + tile, :] = jnp.where(state_lane(2 * head + 1), total, kept)

        if arrays == 1:
            visit(0, None)
            return
        for first in (0, 1):

            @pl.when(parity == first)
            def _(first=first):
                visit(first, None)
                visit(1 - first, q_sources[first])

    def finish(slots, head, pick):
        for n, (q_ref, old_ref, o_ref) in enumerate(zip(q_refs, old_refs, o_refs)):

            def go(q_ref=q_ref, o_ref=o_ref, n=n):
                query_block = block_of(q_sources[n])
                for t in range(0, rows, tile):
                    ml = ml_in[t : t + tile, :]
                    before = [
                        jnp.sum(jnp.where(state_lane(2 * head + i), ml, 0.0), axis=1, keepdims=True)
                        for i in (0, 1)
                    ]
                    before.append(acc_in[t : t + tile, lanes(head)])
                    spans = [
                        (*pick(slot, rows), None, joined(block_of(source), query_block))
                        for slot, source in zip(slots, sources)
                    ]
                    _, total, acc = soften(q_ref[t : t + tile, lanes(head)], spans, before)
                    o_ref[t : t + tile, lanes(head)] = (acc / total).astype(jnp.bfloat16)

            if arrays == 1:
                go()
            else:
                pl.when(parity == n)(go)

                @pl.when(parity != n)
                def _(old_ref=old_ref, o_ref=o_ref):
                    o_ref[:, lanes(head)] = old_ref[:, lanes(head)]

    if mode == "begin":
        states[0][...] = jnp.zeros(states[0].shape, jnp.float32)
    over_heads(finish if mode == "finish" else begin)


def attend(scalars, q_list, kv_list, groups, sources, q_sources, tile, mode, state=()):
    rows, wide = q_list[0].shape
    arrays = len(q_list)
    smem = pl.BlockSpec(memory_space=pltpu.SMEM)
    vmem = pl.BlockSpec(memory_space=pltpu.VMEM)
    heads = sum(g[0] for g in groups)
    operands = [*q_list, *kv_list, *state]
    out_shape = [jax.ShapeDtypeStruct((rows, wide), jnp.bfloat16)] * arrays
    if mode == "begin":
        out_shape += [
            jax.ShapeDtypeStruct((rows, d * HEAD_DIM), jnp.float32) for d in (1, heads)
        ]
    return pl.pallas_call(
        functools.partial(
            attend_kernel,
            arrays=arrays,
            groups=tuple(groups),
            sources=tuple(sources),
            q_sources=tuple(q_sources),
            tile=min(tile, rows),
            mode=mode,
        ),
        out_shape=out_shape,
        in_specs=[smem] * len(scalars) + [vmem] * len(operands),
        out_specs=[vmem] * len(out_shape),
        compiler_params=pltpu.CompilerParams(vmem_limit_bytes=VMEM_LIMIT),
        name="attend",
    )(*scalars, *operands)


def project_call(places, base, pieces, w_blocks, first, out_type):
    rows, own = base.shape
    half = own // 2

    def kernel(places_ref, base_ref, *refs):
        near_refs, refs = refs[: len(pieces)], refs[len(pieces) :]
        w_refs, o_refs = refs[: len(w_blocks)], refs[len(w_blocks) : -1]
        context_ref = refs[-1]
        side = lax.rem(places_ref[0], 2)
        for step, ref in enumerate(near_refs):
            block, other = divmod(step, 2)
            at = block * own + (side if other == 0 else 1 - side) * half
            context_ref[:, pl.ds(pl.multiple_of(at, half), half)] = ref[...]
        total = base_ref[...].astype(jnp.float32)
        for block, w_ref in enumerate(w_refs):
            total += jnp.dot(
                context_ref[:, block * own : (block + 1) * own],
                w_ref[...],
                preferred_element_type=jnp.float32,
            )
        total = total.astype(out_type)
        o_refs[0][...] = total
        for n, ref in enumerate(o_refs[1:]):
            ref[...] = total[n * cut : (n + 1) * cut]

    cut = rows // 2
    shapes = [base.shape] if first else [base.shape, (cut, own), (cut, own)]
    whole = lambda a: pl.BlockSpec(a.shape, lambda i, places_ref: (0, 0))
    corner = pl.BlockSpec((own, own), lambda i, places_ref: (0, places_ref[1] if first else 0))
    return pl.pallas_call(
        kernel,
        grid_spec=pltpu.PrefetchScalarGridSpec(
            num_scalar_prefetch=1,
            grid=(1,),
            in_specs=[whole(a) for a in (base, *pieces)]
            + [corner]
            + [whole(w) for w in w_blocks[1:]],
            out_specs=[pl.BlockSpec(s, lambda i, places_ref: (0, 0)) for s in shapes],
            scratch_shapes=[pltpu.VMEM((rows, own * len(w_blocks)), jnp.bfloat16)],
        ),
        out_shape=[jax.ShapeDtypeStruct(s, out_type) for s in shapes],
        compiler_params=pltpu.CompilerParams(vmem_limit_bytes=VMEM_LIMIT),
        name="project",
    )(places, base, *pieces, *w_blocks)


def norm_into(lane, gain_ref, pieces, at_row, normed_ref):
    wide = pieces[0][0].shape[1]
    rows = pieces[0][1].stop - pieces[0][1].start
    total = 0.0
    for ref, part in pieces:
        x = ref[part, :].astype(jnp.float32)
        total += jnp.sum(x * x, axis=1, keepdims=True)
    scale = lax.rsqrt(total / (wide * len(pieces)) + EPSILON)
    for step, (ref, part) in enumerate(pieces):
        at = pl.multiple_of((lane ^ step) * wide, wide)
        x = ref[part, :].astype(jnp.float32)
        normed_ref[at_row : at_row + rows, pl.ds(at, wide)] = (
            x * scale * gain_ref[:, pl.ds(at, wide)]
        ).astype(jnp.bfloat16)


def fetch(place_ref, pieces, buffer, sems, rings):
    z = place_ref[0] // 2
    for k in range(rings):

        def begin(name, k=k):
            pltpu.make_async_copy(pieces[name], buffer.at[k], sems.at[k]).start()

        if k == 0:
            begin(("w", 0))
        else:

            @pl.when(z >= k)
            def _(k=k, begin=begin):
                begin(("up", k))

            @pl.when(z < k)
            def _(k=k, begin=begin):
                begin(("down", rings - k))


def gather_dot(place_ref, normed, pieces, buffer, sems, rings):
    z = place_ref[0] // 2
    depth = buffer.shape[1]
    total = 0.0
    for k in range(rings):
        if sems is not None:
            pltpu.make_async_copy(pieces[("w", 0)], buffer.at[k], sems.at[k]).wait()
        at = pl.multiple_of(lax.rem(z - k + rings, rings) * depth, depth)
        total += jnp.dot(normed[:, pl.ds(at, depth)], buffer[k], preferred_element_type=jnp.float32)
    return total


def cache_call(place1, lane1, gain, hiddens, pieces, rings):
    names = list(pieces)
    depth, width = pieces[("w", 0)].shape
    arrays = [a for _, group in hiddens for a, _ in group]
    total = sum(part.stop - part.start for _, ((_, part), *_) in hiddens)
    wide = arrays[0].shape[1] * len(hiddens[0][1])

    def kernel(place_ref, lane_ref, gain_ref, *refs):
        hidden_refs = refs[: len(arrays)]
        piece_refs = refs[len(arrays) : len(arrays) + len(names)]
        normed_ref, cache_ref, buffer, sems = refs[len(arrays) + len(names) :]
        at = dict(zip(names, piece_refs))
        fetch(place_ref, at, buffer, sems, rings)
        taken = 0
        for row, group in hiddens:
            pairs = [(hidden_refs[taken + n], part) for n, (_, part) in enumerate(group)]
            taken += len(group)
            norm_into(lane_ref[0], gain_ref, pairs, row, normed_ref)
        cache_ref[...] = gather_dot(place_ref, normed_ref, at, buffer, sems, rings).astype(
            jnp.bfloat16
        )

    vmem = pl.BlockSpec(memory_space=pltpu.VMEM)
    smem = pl.BlockSpec(memory_space=pltpu.SMEM)
    return pl.pallas_call(
        kernel,
        out_shape=[
            jax.ShapeDtypeStruct((total, wide), jnp.bfloat16),
            jax.ShapeDtypeStruct((total, width), jnp.bfloat16),
        ],
        in_specs=[smem, smem, vmem]
        + [vmem] * len(arrays)
        + [pl.BlockSpec(memory_space=pl.ANY)] * len(names),
        out_specs=[vmem] * 2,
        scratch_shapes=[
            pltpu.VMEM((rings, depth, width), jnp.bfloat16),
            pltpu.SemaphoreType.DMA((rings,)),
        ],
        compiler_params=pltpu.CompilerParams(vmem_limit_bytes=PROJECT_LIMIT),
        name="cache",
    )(place1, lane1, gain, *arrays, *[pieces[n] for n in names])


def query_call(place1, normed, pieces, rings):
    names = list(pieces)
    depth, width = pieces[("w", 0)].shape
    count = len(normed)

    def kernel(place_ref, *refs):
        normed_refs, refs = refs[:count], refs[count:]
        piece_refs, refs = refs[: len(names)], refs[len(names) :]
        o_refs, (buffer, sems) = refs[:count], refs[count:]
        at = dict(zip(names, piece_refs))
        fetch(place_ref, at, buffer, sems, rings)
        for n in range(count):
            o_refs[n][...] = gather_dot(
                place_ref, normed_refs[n], at, buffer, None if n else sems, rings
            ).astype(jnp.bfloat16)

    vmem = pl.BlockSpec(memory_space=pltpu.VMEM)
    return pl.pallas_call(
        kernel,
        out_shape=[jax.ShapeDtypeStruct((a.shape[0], width), jnp.bfloat16) for a in normed],
        in_specs=[pl.BlockSpec(memory_space=pltpu.SMEM)]
        + [vmem] * count
        + [pl.BlockSpec(memory_space=pl.ANY)] * len(names),
        out_specs=[vmem] * count,
        scratch_shapes=[
            pltpu.VMEM((rings, depth, width), jnp.bfloat16),
            pltpu.SemaphoreType.DMA((rings,)),
        ],
        compiler_params=pltpu.CompilerParams(vmem_limit_bytes=PROJECT_LIMIT),
        name="queries",
    )(place1, *normed, *[pieces[n] for n in names])


def paired_layer(
    residual,
    q_self,
    k_self,
    v_self,
    w_out,
    norm_gain,
    w_query,
    w_cache,
    block_doc,
    tail_len,
    *,
    seq,
    head,
):
    rows, own = residual.shape
    half = own // 2
    parts = half // HEAD_DIM
    rings = seq // 2
    place = lax.axis_index("seq").astype(jnp.int32)
    lane = lax.axis_index("head").astype(jnp.int32)
    side = lax.rem(place, 2)
    place1, lane1 = place[None], lane[None]

    def send(block, axis, target, source=None):
        size = seq if axis == "seq" else head
        return moved(
            block, axis, size, lambda i: target(i) if source is None or source(i) else None
        )

    up = lambda i: i + 2
    down = lambda i: i - 2
    swap = lambda i: i ^ 1
    column = lambda a, at, size: lax.dynamic_slice_in_dim(a, at, size, 1)

    def kv_of(which):
        at = which * half
        return jnp.concatenate([column(k_self, at, half), column(v_self, at, half)], axis=1)

    mine, theirs = kv_of(side), kv_of(1 - side)
    q_mine = column(q_self, side * half, half)
    q_theirs = column(q_self, (1 - side) * half, half)
    above = send(mine, "seq", up)
    near = send(theirs, "seq", swap)
    across = send(near, "seq", up)
    odd = jnp.where(side == 1, above, across)
    far = send(odd, "seq", up, lambda i: i >= 2)
    q_near = send(q_theirs, "seq", swap)

    w_blocks = [w_out]
    late = lax.optimization_barrier(w_out)
    for step in (2, 1, 3):
        source = late if step == 1 else w_out
        piece = lax.dynamic_slice_in_dim(source, (lane ^ step) * own, own, 1)
        w_blocks.append(send(piece, "head", lambda i: i ^ step))

    kv_width = w_cache.shape[1] // 2
    kv_half = kv_width // 2

    def columns_of(which):
        return jnp.concatenate(
            [
                column(w_cache, which * kv_half, kv_half),
                column(w_cache, kv_width + which * kv_half, kv_half),
                column(w_query, which * half, half),
            ],
            axis=1,
        )

    def ordered(kept, got, axis):
        return jnp.where(
            side == 0,
            jnp.concatenate([kept, got], axis=axis),
            jnp.concatenate([got, kept], axis=axis),
        )

    w_kept = columns_of(side)
    w_got = send(columns_of(1 - side), "seq", swap)
    tables = []
    for name, start, stop in (("c", 0, kv_width), ("q", kv_width, kv_width + half)):
        w = ordered(w_kept[:, start:stop], w_got[:, start:stop], 0)
        table = {("w", 0): w}
        high = low = w
        for k in range(1, rings):
            high = send(high, "seq", up, lambda i: i // 2 >= k - 1)
            if name == "c" or k == rings - 1:
                low = send(w, "seq", lambda i: i - 2 * k)
            else:
                low = send(low, "seq", down, lambda i: i // 2 <= rings - k)
            table[("up", k)] = high
            table[("down", k)] = low
        tables.append(table)
    cache_pieces, query_pieces = tables

    scalars = (place1, block_doc, tail_len)
    pair = [("back", 0), ("pair", 0)]
    o_mine, o_theirs, *state = attend(
        scalars,
        [q_mine, q_near],
        [mine, near, above, across],
        [(parts, False)],
        pair + [("back", 2), ("pair", 2)],
        pair,
        SELF_TILE,
        "begin",
    )
    o_mine, o_theirs = attend(
        scalars,
        [q_mine, q_near],
        [far],
        [(parts, False)],
        [("odd", 2)],
        pair,
        SELF_TILE,
        "finish",
        [*state, o_mine, o_theirs],
    )
    both = lambda i: ((i // head) ^ 1) * head + ((i % head) ^ 2)
    route = [(i, both(i)) for i in range(seq * head)]
    corner = lax.ppermute(o_theirs, ("seq", "head"), route)
    flip = lambda i: i ^ 1
    places = jnp.stack([place, lane])
    contexts = [o_mine, send(o_theirs, "seq", swap), send(o_mine, "head", lambda i: i ^ 2), corner]
    others = [send(piece, "head", flip) for piece in contexts]
    (partial,) = project_call(
        places,
        residual,
        contexts[:2] + others[:2],
        [w_blocks[0], w_blocks[2]],
        True,
        jnp.float32,
    )
    hidden, hidden_low, hidden_high = project_call(
        places,
        partial,
        contexts[2:] + others[2:],
        [w_blocks[1], w_blocks[3]],
        False,
        jnp.bfloat16,
    )
    beside = lambda i: i ^ 2
    x_low = send(hidden_low, "head", beside)
    y_high = send(hidden_high, "seq", swap)
    x_high = send(hidden_high, "head", beside)
    y_low = send(hidden_low, "seq", swap)
    corner_low = send(x_low, "seq", swap)
    corner_high = send(y_high, "head", beside)
    own_core = send(hidden, "head", flip)
    core = [
        send(piece, "head", flip)
        for piece in (x_low, x_high, y_low, y_high, corner_low, corner_high)
    ]
    cut = rows // 2
    whole, low_rows, high_rows = slice(0, cut), slice(0, cut), slice(cut, rows)
    gain = norm_gain[None, :]
    groups = [
        (0, [(hidden, low_rows), (own_core, low_rows), (x_low, whole), (core[0], whole)]),
        (cut, [(hidden, high_rows), (own_core, high_rows), (x_high, whole), (core[1], whole)]),
    ]
    normed_mine, cache_mine = cache_call(place1, lane1, gain, groups, cache_pieces, rings)
    groups = [
        (0, [(a, whole) for a in (y_low, core[2], corner_low, core[4])]),
        (cut, [(a, whole) for a in (y_high, core[3], corner_high, core[5])]),
    ]
    normed_near, cache_near = cache_call(place1, lane1, gain, groups, cache_pieces, rings)
    q_pair = query_call(place1, [normed_mine, normed_near], query_pieces, rings)
    cache_above = send(cache_mine, "seq", up)
    cache_across = send(cache_near, "seq", up)
    cache_odd = jnp.where(side == 1, cache_above, cache_across)
    cache_far = send(cache_odd, "seq", up, lambda i: i >= 2)
    o_mine, o_theirs, *state = attend(
        scalars,
        q_pair,
        [cache_mine, cache_near, cache_above, cache_across],
        [(parts, True)],
        pair + [("back", 2), ("pair", 2)],
        pair,
        CROSS_TILE,
        "begin",
    )
    o_mine, o_theirs = attend(
        scalars,
        q_pair,
        [cache_far],
        [(parts, True)],
        [("odd", 2)],
        pair,
        CROSS_TILE,
        "finish",
        [*state, o_mine, o_theirs],
    )
    cross_context = ordered(o_mine, send(o_theirs, "seq", swap), 1)
    return (hidden, cross_context)


def direct_attend_kernel(
    place_ref, doc_ref, tail_ref, q_ref, *refs, slots, heads, group, q_tile, reach
):
    kv_refs = refs[: len(slots)]
    o_ref, m_ref, l_ref, acc_ref = refs[len(slots) :]
    rows = q_ref.shape[0]
    blocks = doc_ref.shape[0]
    kv_heads = heads // group
    factor = LOG2E / math.sqrt(HEAD_DIM)
    here = place_ref[0]
    own_doc = doc_ref[here]
    after = jnp.minimum(here + 1, blocks - 1)
    closing = jnp.logical_or(here == blocks - 1, doc_ref[after] != own_doc)
    live = jnp.where(closing, tail_ref[here], rows)

    def scores(kv_ref, t, h):
        q = q_ref[pl.ds(t, q_tile), h * HEAD_DIM : (h + 1) * HEAD_DIM]
        g = h // group
        k = kv_ref[:, g * HEAD_DIM : (g + 1) * HEAD_DIM]
        return lax.dot_general(q, k, (((1,), (1,)), ((), ())), preferred_element_type=jnp.float32)

    def values(kv_ref, h):
        g = kv_heads + h // group
        return kv_ref[:, g * HEAD_DIM : (g + 1) * HEAD_DIM]

    def tiles(step):
        def body(i, carry):
            step(pl.multiple_of(i * q_tile, q_tile))
            return carry

        lax.fori_loop(0, rows // q_tile, body, 0)

    def first(t):
        kv_ref = kv_refs[0]
        row = t + lax.broadcasted_iota(jnp.int32, (q_tile, rows), 0)
        col = lax.broadcasted_iota(jnp.int32, (q_tile, rows), 1)
        keep = jnp.logical_and(col <= row, col < live)
        for h in range(heads):
            s = jnp.where(keep, scores(kv_ref, t, h), -1e30)
            m = jnp.max(s, axis=1, keepdims=True)
            p = jnp.exp2((s - m) * factor)
            m_ref[h, pl.ds(t, q_tile), :] = jnp.broadcast_to(m, (q_tile, HEAD_DIM))
            l_ref[h, pl.ds(t, q_tile), :] = jnp.broadcast_to(
                jnp.sum(p, axis=1, keepdims=True), (q_tile, HEAD_DIM)
            )
            acc_ref[h, pl.ds(t, q_tile), :] = jnp.dot(
                p.astype(jnp.bfloat16), values(kv_ref, h), preferred_element_type=jnp.float32
            )

    def later(kv_ref, back):
        def step(t):
            if back * rows + rows - 1 >= reach:
                row = t + lax.broadcasted_iota(jnp.int32, (q_tile, rows), 0)
                col = lax.broadcasted_iota(jnp.int32, (q_tile, rows), 1)
                keep = back * rows + row - col < reach
            else:
                keep = None
            for h in range(heads):
                s = scores(kv_ref, t, h)
                if keep is not None:
                    s = jnp.where(keep, s, -1e30)
                m_old = m_ref[h, pl.ds(t, q_tile), :]
                m = jnp.maximum(m_old, jnp.max(s, axis=1, keepdims=True))
                shrink = jnp.exp2((m_old - m) * factor)
                p = jnp.exp2((s - m[:, :1]) * factor)
                m_ref[h, pl.ds(t, q_tile), :] = m
                l_ref[h, pl.ds(t, q_tile), :] = l_ref[h, pl.ds(t, q_tile), :] * shrink + jnp.sum(
                    p, axis=1, keepdims=True
                )
                acc_ref[h, pl.ds(t, q_tile), :] = acc_ref[
                    h, pl.ds(t, q_tile), :
                ] * shrink + jnp.dot(
                    p.astype(jnp.bfloat16), values(kv_ref, h), preferred_element_type=jnp.float32
                )

        return step

    tiles(first)
    for kv_ref, (even, odd) in zip(kv_refs[1:], slots[1:]):
        parity = lax.rem(here, 2)
        for back, only in ((even, 0), (odd, 1)):
            if back is None or (even == odd and only == 1):
                continue
            source = here - back
            wanted = jnp.logical_and(source >= 0, doc_ref[jnp.maximum(source, 0)] == own_doc)
            if even != odd:
                wanted = jnp.logical_and(wanted, parity == only)
            span = back

            @pl.when(wanted)
            def _(kv_ref=kv_ref, span=span):
                tiles(later(kv_ref, span))

    for h in range(heads):
        o_ref[:, h * HEAD_DIM : (h + 1) * HEAD_DIM] = (acc_ref[h] / l_ref[h]).astype(jnp.bfloat16)


def direct_attend(place, block_doc, tail_len, queries, column_block, heads, kv_list, slots, reach):
    rows, width = kv_list[0].shape
    kv_heads = width // (2 * HEAD_DIM)
    wide = heads * HEAD_DIM
    smem = pl.BlockSpec(memory_space=pltpu.SMEM)
    whole = pl.BlockSpec((rows, width), lambda i: (0, 0))
    return pl.pallas_call(
        functools.partial(
            direct_attend_kernel,
            slots=slots,
            heads=heads,
            group=heads // kv_heads,
            q_tile=min(256, rows),
            reach=reach,
        ),
        grid=(1,),
        out_shape=jax.ShapeDtypeStruct((rows, wide), jnp.bfloat16),
        in_specs=[smem, smem, smem, pl.BlockSpec((rows, wide), lambda i: (0, column_block))]
        + [whole] * len(kv_list),
        out_specs=pl.BlockSpec((rows, wide), lambda i: (0, 0)),
        scratch_shapes=[pltpu.VMEM((heads, rows, HEAD_DIM), jnp.float32)] * 3,
        compiler_params=pltpu.CompilerParams(vmem_limit_bytes=VMEM_LIMIT),
        name="attend",
    )(place, block_doc, tail_len, queries, *kv_list)


def direct_project_kernel(*refs, parts, blocks):
    residual_ref = refs[0]
    context_refs = refs[1 : 1 + parts * blocks]
    w_refs = refs[1 + parts * blocks : 1 + parts * blocks + blocks]
    o_ref = refs[-1]
    total = residual_ref[...].astype(jnp.float32)
    depth = context_refs[0].shape[1]
    for part in range(parts):
        for block in range(blocks):
            total += jnp.dot(
                context_refs[part * blocks + block][...],
                w_refs[block][part * depth : (part + 1) * depth, :],
                preferred_element_type=jnp.float32,
            )
    o_ref[...] = total.astype(jnp.bfloat16)


def norm_kernel(place_ref, gain_ref, *refs, near):
    hidden_refs, o_ref = refs[:-1], refs[-1]
    wide = hidden_refs[0].shape[1]
    total = 0.0
    for ref in hidden_refs:
        x = ref[...].astype(jnp.float32)
        total += jnp.sum(x * x, axis=1, keepdims=True)
    scale = lax.rsqrt(total / (wide * len(hidden_refs)) + EPSILON)
    for step, ref in enumerate(hidden_refs):
        at = pl.multiple_of(near(place_ref[0], step) * wide, wide)
        x = ref[...].astype(jnp.float32)
        o_ref[:, pl.ds(at, wide)] = (x * scale * gain_ref[:, pl.ds(at, wide)]).astype(jnp.bfloat16)


def columns_kernel(order_ref, normed_ref, *refs):
    w_refs, o_ref = refs[:-1], refs[-1]
    depth = w_refs[0].shape[0]
    total = 0.0
    for step, ref in enumerate(w_refs):
        at = pl.multiple_of(order_ref[step] * depth, depth)
        total += jnp.dot(
            normed_ref[:, pl.ds(at, depth)], ref[...], preferred_element_type=jnp.float32
        )
    o_ref[...] = total.astype(jnp.bfloat16)


def simple_call(kernel, out_shape, scalars, arrays):
    return pl.pallas_call(
        kernel,
        out_shape=out_shape,
        in_specs=[pl.BlockSpec(memory_space=pltpu.SMEM)] * len(scalars)
        + [pl.BlockSpec(memory_space=pltpu.VMEM)] * len(arrays),
        out_specs=pl.BlockSpec(memory_space=pltpu.VMEM),
        compiler_params=pltpu.CompilerParams(vmem_limit_bytes=VMEM_LIMIT),
    )(*scalars, *arrays)


def direct_layer(
    residual,
    q_self,
    k_self,
    v_self,
    w_out,
    norm_gain,
    w_query,
    w_cache,
    block_doc,
    tail_len,
    *,
    seq,
    head,
    span,
    paired,
):
    rows, own = residual.shape
    local_heads = q_self.shape[1] // HEAD_DIM
    place = lax.axis_index("seq").astype(jnp.int32)
    lane = lax.axis_index("head").astype(jnp.int32)
    place1, lane1 = place[None], lane[None]

    def along(block, target):
        return moved(block, "seq", seq, target)

    def across(block, step):
        return moved(block, "head", head, lambda i: i ^ step)

    even = lambda i: i % 2 == 0

    def spread(block):
        if not paired:
            return [along(block, lambda i, d=d: i + d) for d in range(1, span)]
        far = along(block, lambda i: i + 2)
        near = along(block, lambda i: i + 1 if even(i) else None)
        swap = along(far, lambda i: i ^ 1)
        last = along(swap, lambda i: i + 2 if even(i) else None)
        return [far, near, swap, last]

    if paired:
        slots = ((0, 0), (2, 2), (None, 1), (1, 3), (3, None))
    else:
        slots = tuple((d, d) for d in range(span))

    parts = local_heads // 2
    per = local_heads // parts
    width = per * HEAD_DIM
    kv_parts = []
    for c in range(parts):
        cols = slice(c * width, (c + 1) * width)
        own_kv = jnp.concatenate([k_self[:, cols], v_self[:, cols]], axis=1)
        kv_parts.append([own_kv] + spread(own_kv))

    w_blocks = []
    for step in range(head):
        piece = lax.dynamic_slice_in_dim(w_out, (lane ^ step) * own, own, 1)
        w_blocks.append(piece if step == 0 else across(piece, step))

    def gathered(w):
        if not paired:
            whole = lax.all_gather(w, "seq", axis=0, tiled=True)
            return [whole]
        pieces = [w, along(w, lambda i: i ^ 1)]
        ring = list(pieces)
        for distance in range(1, seq // 2):
            if distance <= seq // 4:
                ring = [along(p, lambda i: (i - 2) % seq) for p in ring]
                pieces += ring
            else:
                pieces += [
                    along(p, lambda i: (i + 2 * (seq // 2 - distance)) % seq) for p in pieces[:2]
                ]
        return pieces

    if paired:
        order = [(place ^ y) + 2 * distance for distance in range(seq // 2) for y in (0, 1)]
        order = jnp.stack([lax.rem(o, seq) for o in order])
    else:
        order = jnp.zeros((1,), jnp.int32)
    cache_w = gathered(w_cache)
    query_w = gathered(w_query)

    contexts = []
    for c in range(parts):
        mine = direct_attend(
            place1, block_doc, tail_len, q_self, c, per, kv_parts[c], slots, WINDOW
        )
        pair = [mine, across(mine, 2)]
        other = [across(p, 1) for p in pair]
        contexts += [pair[0], other[0], pair[1], other[1]]
    hidden = simple_call(
        functools.partial(direct_project_kernel, parts=parts, blocks=head),
        jax.ShapeDtypeStruct((rows, own), jnp.bfloat16),
        [],
        [residual, *contexts, *w_blocks],
    )
    pair = [hidden, across(hidden, 2)]
    other = [across(p, 1) for p in pair]
    normed = simple_call(
        functools.partial(norm_kernel, near=lambda at, step: at ^ step),
        jax.ShapeDtypeStruct((rows, own * head), jnp.bfloat16),
        [lane1],
        [norm_gain[None, :], pair[0], other[0], pair[1], other[1]],
    )
    cache = simple_call(
        columns_kernel,
        jax.ShapeDtypeStruct((rows, w_cache.shape[1]), jnp.bfloat16),
        [order],
        [normed, *cache_w],
    )
    history = [cache] + spread(cache)
    cross_queries = simple_call(
        columns_kernel,
        jax.ShapeDtypeStruct((rows, w_query.shape[1]), jnp.bfloat16),
        [order],
        [normed, *query_w],
    )
    cross_context = direct_attend(
        place1,
        block_doc,
        tail_len,
        cross_queries,
        0,
        local_heads,
        history,
        slots,
        rows * span,
    )
    return (hidden, cross_context)


def solution(mesh):
    seq, head = mesh.shape["seq"], mesh.shape["head"]
    span = min(5, seq // 2)
    in_specs = (
        P("seq", "head"),
        P("seq", "head"),
        P("seq", "head"),
        P("seq", "head"),
        P("head", None),
        P(),
        P("seq", "head"),
        P("seq", "head"),
        P(),
        P(),
    )
    out_specs = (P("seq", "head"), P("seq", "head"))
    if seq == 2 * span and head == 4:
        layer = functools.partial(paired_layer, seq=seq, head=head)
    else:
        layer = functools.partial(direct_layer, seq=seq, head=head, span=span, paired=False)

    def body(*args):
        return layer(*args)

    return jax.shard_map(body, mesh=mesh, in_specs=in_specs, out_specs=out_specs, check_vma=False)
```

```python
import functools
import math

import jax
import jax.numpy as jnp
from jax import lax
from jax.experimental import pallas as pl
from jax.experimental.pallas import tpu as pltpu
from jax.sharding import PartitionSpec as P


HEAD_DIM = 128
WINDOW = 2048
EPSILON = 1e-06
SELF_TILE = 256
VMEM_LIMIT = 24 * 2**20
PROJECT_LIMIT = 32 * 2**20
CROSS_TILE = 256
LOG2E = 1.4426950408889634


def moved(block, axis, size, target):
    route = [(i, target(i)) for i in range(size)]
    route = [(i, j) for i, j in route if j is not None and 0 <= j < size]
    return lax.ppermute(block, axis, route)


def attend_kernel(
    place_ref, doc_ref, tail_ref, *refs, arrays, groups, sources, q_sources, tile, mode
):
    count = len(sources) * len(groups)
    q_refs, refs = refs[:arrays], refs[arrays:]
    kv_refs, refs = refs[:count], refs[count:]
    if mode == "finish":
        ml_in, acc_in, *old_refs = refs[: 2 + arrays]
        o_refs = refs[2 + arrays :]
    else:
        o_refs, states = refs[:arrays], refs[arrays:]
    rows = q_refs[0].shape[0]
    blocks = doc_ref.shape[0]
    factor = LOG2E / math.sqrt(HEAD_DIM)
    here = place_ref[0]
    parity = lax.rem(here, 2)

    def lanes(at):
        if isinstance(at, int):
            return slice(at * HEAD_DIM, (at + 1) * HEAD_DIM)
        return pl.ds(pl.multiple_of(at * HEAD_DIM, HEAD_DIM), HEAD_DIM)

    def block_of(source):
        if source[0] == "back":
            return here - source[1]
        if source[0] == "pair":
            return here + 1 - 2 * parity - source[1]
        return here - parity - 1 - source[1]

    def joined(key_block, query_block):
        safe = jnp.maximum(key_block, 0)
        wanted = jnp.logical_and(key_block >= 0, key_block < query_block)
        return jnp.logical_and(wanted, doc_ref[safe] == doc_ref[query_block])

    def live_rows(block):
        after = jnp.minimum(block + 1, blocks - 1)
        closing = jnp.logical_or(block == blocks - 1, doc_ref[after] != doc_ref[block])
        return jnp.where(closing, tail_ref[block], rows)

    def soften(q, spans, before):
        k = jnp.concatenate([k for k, _, _, _ in spans], axis=0)
        v = jnp.concatenate([v for _, v, _, _ in spans], axis=0)
        v = jnp.concatenate([v, jnp.ones(v.shape, v.dtype)], axis=1)
        s_all = lax.dot_general(q, k, (((1,), (1,)), ((), ())), preferred_element_type=jnp.float32)
        parts, at = [], 0
        m = None if before is None else before[0]
        for k, _, keep, open_span in spans:
            s = s_all[:, at : at + k.shape[0]]
            at += k.shape[0]
            if keep is not None:
                s = jnp.where(keep, s, -1e30)
            peak = jnp.max(s, axis=1, keepdims=True)
            if open_span is not None:
                peak = jnp.where(open_span, peak, -1e30)
            m = peak if m is None else jnp.maximum(m, peak)
            parts.append((s, open_span))
        weights = []
        for s, open_span in parts:
            top = m if open_span is None else jnp.where(open_span, m, 1e30)
            weights.append(jnp.exp2((s - top) * factor).astype(jnp.bfloat16))
        acc = jnp.dot(
            jnp.concatenate(weights, axis=1), v, preferred_element_type=jnp.float32
        )
        if before is not None:
            shrink = jnp.exp2((before[0] - m) * factor)
            return m, acc[:, HEAD_DIM:] + before[1] * shrink, acc[:, :HEAD_DIM] + before[2] * shrink
        return m, acc[:, HEAD_DIM:], acc[:, :HEAD_DIM]

    def state_lane(index):
        return lax.broadcasted_iota(jnp.int32, (tile, HEAD_DIM), 1) == index

    def over_heads(body):
        for g, (heads, shared) in enumerate(groups):
            slots = kv_refs[g * len(sources) : (g + 1) * len(sources)]
            kv_heads = slots[0].shape[1] // (2 * HEAD_DIM)

            def one(h, carry, g=g, heads=heads, shared=shared, slots=slots, kv_heads=kv_heads):
                at = 0 if shared else h

                def pick(slot, keys):
                    return slot[:keys, lanes(at)], slot[:keys, lanes(kv_heads + at)]

                body(slots, g * heads + h, pick)
                return carry

            lax.fori_loop(0, heads, one, 0)

    def begin(slots, head, pick):
        def visit(n, extra):
            query_block = block_of(q_sources[n])
            live = live_rows(query_block)
            for t in range(0, rows, tile):
                keys = t + tile
                row = t + lax.broadcasted_iota(jnp.int32, (tile, keys), 0)
                col = lax.broadcasted_iota(jnp.int32, (tile, keys), 1)
                keep = jnp.logical_and(col <= row, col < live)
                spans = [(*pick(slots[sources.index(q_sources[n])], keys), keep, None)]
                for slot, source in zip(slots, sources):
                    if source not in q_sources or source == extra:
                        spans.append((*pick(slot, rows), None, joined(block_of(source), query_block)))
                m, total, acc = soften(q_refs[n][t : t + tile, lanes(head)], spans, None)
                o_refs[n][t : t + tile, lanes(head)] = (acc / total).astype(jnp.bfloat16)
                if arrays == 1 or extra is None:
                    ml_out, acc_out = states
                    acc_out[t : t + tile, lanes(head)] = acc
                    kept = jnp.where(state_lane(2 * head), m, ml_out[t : t + tile, :])
                    ml_out[t : t + tile, :] = jnp.where(state_lane(2 * head + 1), total, kept)

        if arrays == 1:
            visit(0, None)
            return
        for first in (0, 1):

            @pl.when(parity == first)
            def _(first=first):
                visit(first, None)
                visit(1 - first, q_sources[first])

    def finish(slots, head, pick):
        for n, (q_ref, old_ref, o_ref) in enumerate(zip(q_refs, old_refs, o_refs)):

            def go(q_ref=q_ref, o_ref=o_ref, n=n):
                query_block = block_of(q_sources[n])
                for t in range(0, rows, tile):
                    ml = ml_in[t : t + tile, :]
                    before = [
                        jnp.sum(jnp.where(state_lane(2 * head + i), ml, 0.0), axis=1, keepdims=True)
                        for i in (0, 1)
                    ]
                    before.append(acc_in[t : t + tile, lanes(head)])
                    spans = [
                        (*pick(slot, rows), None, joined(block_of(source), query_block))
                        for slot, source in zip(slots, sources)
                    ]
                    _, total, acc = soften(q_ref[t : t + tile, lanes(head)], spans, before)
                    o_ref[t : t + tile, lanes(head)] = (acc / total).astype(jnp.bfloat16)

            if arrays == 1:
                go()
            else:
                pl.when(parity == n)(go)

                @pl.when(parity != n)
                def _(old_ref=old_ref, o_ref=o_ref):
                    o_ref[:, lanes(head)] = old_ref[:, lanes(head)]

    if mode == "begin":
        states[0][...] = jnp.zeros(states[0].shape, jnp.float32)
    over_heads(finish if mode == "finish" else begin)


def attend(scalars, q_list, kv_list, groups, sources, q_sources, tile, mode, state=()):
    rows, wide = q_list[0].shape
    arrays = len(q_list)
    smem = pl.BlockSpec(memory_space=pltpu.SMEM)
    vmem = pl.BlockSpec(memory_space=pltpu.VMEM)
    heads = sum(g[0] for g in groups)
    operands = [*q_list, *kv_list, *state]
    out_shape = [jax.ShapeDtypeStruct((rows, wide), jnp.bfloat16)] * arrays
    if mode == "begin":
        out_shape += [
            jax.ShapeDtypeStruct((rows, d * HEAD_DIM), jnp.float32) for d in (1, heads)
        ]
    return pl.pallas_call(
        functools.partial(
            attend_kernel,
            arrays=arrays,
            groups=tuple(groups),
            sources=tuple(sources),
            q_sources=tuple(q_sources),
            tile=min(tile, rows),
            mode=mode,
        ),
        out_shape=out_shape,
        in_specs=[smem] * len(scalars) + [vmem] * len(operands),
        out_specs=[vmem] * len(out_shape),
        compiler_params=pltpu.CompilerParams(vmem_limit_bytes=VMEM_LIMIT),
        name="attend",
    )(*scalars, *operands)


def project_call(places, base, pieces, w_blocks, first, out_type):
    rows, own = base.shape
    half = own // 2

    def kernel(places_ref, base_ref, *refs):
        near_refs, refs = refs[: len(pieces)], refs[len(pieces) :]
        w_refs, o_refs = refs[: len(w_blocks)], refs[len(w_blocks) : -1]
        context_ref = refs[-1]
        side = lax.rem(places_ref[0], 2)
        for step, ref in enumerate(near_refs):
            block, other = divmod(step, 2)
            at = block * own + (side if other == 0 else 1 - side) * half
            context_ref[:, pl.ds(pl.multiple_of(at, half), half)] = ref[...]
        total = base_ref[...].astype(jnp.float32)
        for block, w_ref in enumerate(w_refs):
            total += jnp.dot(
                context_ref[:, block * own : (block + 1) * own],
                w_ref[...],
                preferred_element_type=jnp.float32,
            )
        total = total.astype(out_type)
        o_refs[0][...] = total
        for n, ref in enumerate(o_refs[1:]):
            ref[...] = total[n * cut : (n + 1) * cut]

    cut = rows // 2
    shapes = [base.shape] if first else [base.shape, (cut, own), (cut, own)]
    whole = lambda a: pl.BlockSpec(a.shape, lambda i, places_ref: (0, 0))
    corner = pl.BlockSpec((own, own), lambda i, places_ref: (0, places_ref[1] if first else 0))
    return pl.pallas_call(
        kernel,
        grid_spec=pltpu.PrefetchScalarGridSpec(
            num_scalar_prefetch=1,
            grid=(1,),
            in_specs=[whole(a) for a in (base, *pieces)]
            + [corner]
            + [whole(w) for w in w_blocks[1:]],
            out_specs=[pl.BlockSpec(s, lambda i, places_ref: (0, 0)) for s in shapes],
            scratch_shapes=[pltpu.VMEM((rows, own * len(w_blocks)), jnp.bfloat16)],
        ),
        out_shape=[jax.ShapeDtypeStruct(s, out_type) for s in shapes],
        compiler_params=pltpu.CompilerParams(vmem_limit_bytes=VMEM_LIMIT),
        name="project",
    )(places, base, *pieces, *w_blocks)


def norm_into(lane, gain_ref, pieces, at_row, normed_ref):
    wide = pieces[0][0].shape[1]
    rows = pieces[0][1].stop - pieces[0][1].start
    total = 0.0
    for ref, part in pieces:
        x = ref[part, :].astype(jnp.float32)
        total += jnp.sum(x * x, axis=1, keepdims=True)
    scale = lax.rsqrt(total / (wide * len(pieces)) + EPSILON)
    for step, (ref, part) in enumerate(pieces):
        at = pl.multiple_of((lane ^ step) * wide, wide)
        x = ref[part, :].astype(jnp.float32)
        normed_ref[at_row : at_row + rows, pl.ds(at, wide)] = (
            x * scale * gain_ref[:, pl.ds(at, wide)]
        ).astype(jnp.bfloat16)


def fetch(place_ref, pieces, buffer, sems, rings):
    z = place_ref[0] // 2
    for k in range(rings):

        def begin(name, k=k):
            pltpu.make_async_copy(pieces[name], buffer.at[k], sems.at[k]).start()

        if k == 0:
            begin(("w", 0))
        else:

            @pl.when(z >= k)
            def _(k=k, begin=begin):
                begin(("up", k))

            @pl.when(z < k)
            def _(k=k, begin=begin):
                begin(("down", rings - k))


def gather_dot(place_ref, normed, pieces, buffer, sems, rings):
    z = place_ref[0] // 2
    depth = buffer.shape[1]
    total = 0.0
    for k in range(rings):
        if sems is not None:
            pltpu.make_async_copy(pieces[("w", 0)], buffer.at[k], sems.at[k]).wait()
        at = pl.multiple_of(lax.rem(z - k + rings, rings) * depth, depth)
        total += jnp.dot(normed[:, pl.ds(at, depth)], buffer[k], preferred_element_type=jnp.float32)
    return total


def cache_call(place1, lane1, gain, hiddens, pieces, rings):
    names = list(pieces)
    depth, width = pieces[("w", 0)].shape
    arrays = [a for _, group in hiddens for a, _ in group]
    total = sum(part.stop - part.start for _, ((_, part), *_) in hiddens)
    wide = arrays[0].shape[1] * len(hiddens[0][1])

    def kernel(place_ref, lane_ref, gain_ref, *refs):
        hidden_refs = refs[: len(arrays)]
        piece_refs = refs[len(arrays) : len(arrays) + len(names)]
        normed_ref, cache_ref, buffer, sems = refs[len(arrays) + len(names) :]
        at = dict(zip(names, piece_refs))
        fetch(place_ref, at, buffer, sems, rings)
        taken = 0
        for row, group in hiddens:
            pairs = [(hidden_refs[taken + n], part) for n, (_, part) in enumerate(group)]
            taken += len(group)
            norm_into(lane_ref[0], gain_ref, pairs, row, normed_ref)
        cache_ref[...] = gather_dot(place_ref, normed_ref, at, buffer, sems, rings).astype(
            jnp.bfloat16
        )

    vmem = pl.BlockSpec(memory_space=pltpu.VMEM)
    smem = pl.BlockSpec(memory_space=pltpu.SMEM)
    return pl.pallas_call(
        kernel,
        out_shape=[
            jax.ShapeDtypeStruct((total, wide), jnp.bfloat16),
            jax.ShapeDtypeStruct((total, width), jnp.bfloat16),
        ],
        in_specs=[smem, smem, vmem]
        + [vmem] * len(arrays)
        + [pl.BlockSpec(memory_space=pl.ANY)] * len(names),
        out_specs=[vmem] * 2,
        scratch_shapes=[
            pltpu.VMEM((rings, depth, width), jnp.bfloat16),
            pltpu.SemaphoreType.DMA((rings,)),
        ],
        compiler_params=pltpu.CompilerParams(vmem_limit_bytes=PROJECT_LIMIT),
        name="cache",
    )(place1, lane1, gain, *arrays, *[pieces[n] for n in names])


def query_call(place1, normed, pieces, rings):
    names = list(pieces)
    depth, width = pieces[("w", 0)].shape
    count = len(normed)

    def kernel(place_ref, *refs):
        normed_refs, refs = refs[:count], refs[count:]
        piece_refs, refs = refs[: len(names)], refs[len(names) :]
        o_refs, (buffer, sems) = refs[:count], refs[count:]
        at = dict(zip(names, piece_refs))
        fetch(place_ref, at, buffer, sems, rings)
        for n in range(count):
            o_refs[n][...] = gather_dot(
                place_ref, normed_refs[n], at, buffer, None if n else sems, rings
            ).astype(jnp.bfloat16)

    vmem = pl.BlockSpec(memory_space=pltpu.VMEM)
    return pl.pallas_call(
        kernel,
        out_shape=[jax.ShapeDtypeStruct((a.shape[0], width), jnp.bfloat16) for a in normed],
        in_specs=[pl.BlockSpec(memory_space=pltpu.SMEM)]
        + [vmem] * count
        + [pl.BlockSpec(memory_space=pl.ANY)] * len(names),
        out_specs=[vmem] * count,
        scratch_shapes=[
            pltpu.VMEM((rings, depth, width), jnp.bfloat16),
            pltpu.SemaphoreType.DMA((rings,)),
        ],
        compiler_params=pltpu.CompilerParams(vmem_limit_bytes=PROJECT_LIMIT),
        name="queries",
    )(place1, *normed, *[pieces[n] for n in names])


def beside_call(which, a, b):
    rows, wide = a.shape
    half = wide // 2

    def kernel(which_ref, a_ref, b_ref, o_ref, sems):
        part = pl.ds(pl.multiple_of(which_ref[0] * half, HEAD_DIM), half)
        copies = [
            pltpu.make_async_copy(
                ref.at[:, part], o_ref.at[:, n * half : (n + 1) * half], sems.at[n]
            )
            for n, ref in enumerate((a_ref, b_ref))
        ]
        for copy in copies:
            copy.start()
        for copy in copies:
            copy.wait()

    anywhere = pl.BlockSpec(memory_space=pl.ANY)
    return pl.pallas_call(
        kernel,
        out_shape=jax.ShapeDtypeStruct((rows, wide), a.dtype),
        in_specs=[pl.BlockSpec(memory_space=pltpu.SMEM), anywhere, anywhere],
        out_specs=anywhere,
        scratch_shapes=[pltpu.SemaphoreType.DMA((2,))],
        name="beside",
    )(which, a, b)


def paired_layer(
    residual,
    q_self,
    k_self,
    v_self,
    w_out,
    norm_gain,
    w_query,
    w_cache,
    block_doc,
    tail_len,
    *,
    seq,
    head,
):
    rows, own = residual.shape
    half = own // 2
    parts = half // HEAD_DIM
    rings = seq // 2
    place = lax.axis_index("seq").astype(jnp.int32)
    lane = lax.axis_index("head").astype(jnp.int32)
    side = lax.rem(place, 2)
    place1, lane1 = place[None], lane[None]

    def send(block, axis, target, source=None):
        size = seq if axis == "seq" else head
        return moved(
            block, axis, size, lambda i: target(i) if source is None or source(i) else None
        )

    up = lambda i: i + 2
    down = lambda i: i - 2
    swap = lambda i: i ^ 1
    column = lambda a, at, size: lax.dynamic_slice_in_dim(a, at, size, 1)

    def kv_of(which):
        return beside_call(which[None], k_self, v_self)

    mine, theirs = kv_of(side), kv_of(1 - side)
    q_mine = column(q_self, side * half, half)
    q_theirs = column(q_self, (1 - side) * half, half)
    above = send(mine, "seq", up)
    near = send(theirs, "seq", swap)
    across = send(near, "seq", up)
    odd = jnp.where(side == 1, above, across)
    far = send(odd, "seq", up, lambda i: i >= 2)
    q_near = send(q_theirs, "seq", swap)

    w_blocks = [w_out]
    late = lax.optimization_barrier(w_out)
    for step in (2, 1, 3):
        source = late if step == 1 else w_out
        piece = lax.dynamic_slice_in_dim(source, (lane ^ step) * own, own, 1)
        w_blocks.append(send(piece, "head", lambda i: i ^ step))

    kv_width = w_cache.shape[1] // 2
    kv_half = kv_width // 2

    def columns_of(which):
        return jnp.concatenate(
            [
                column(w_cache, which * kv_half, kv_half),
                column(w_cache, kv_width + which * kv_half, kv_half),
                column(w_query, which * half, half),
            ],
            axis=1,
        )

    def ordered(kept, got, axis):
        return jnp.where(
            side == 0,
            jnp.concatenate([kept, got], axis=axis),
            jnp.concatenate([got, kept], axis=axis),
        )

    w_kept = columns_of(side)
    w_got = send(columns_of(1 - side), "seq", swap)
    tables = []
    for name, start, stop in (("c", 0, kv_width), ("q", kv_width, kv_width + half)):
        w = ordered(w_kept[:, start:stop], w_got[:, start:stop], 0)
        table = {("w", 0): w}
        high = low = w
        for k in range(1, rings):
            high = send(high, "seq", up, lambda i: i // 2 >= k - 1)
            if name == "c" or k == rings - 1:
                low = send(w, "seq", lambda i: i - 2 * k)
            else:
                low = send(low, "seq", down, lambda i: i // 2 <= rings - k)
            table[("up", k)] = high
            table[("down", k)] = low
        tables.append(table)
    cache_pieces, query_pieces = tables

    scalars = (place1, block_doc, tail_len)
    pair = [("back", 0), ("pair", 0)]
    o_mine, o_theirs, *state = attend(
        scalars,
        [q_mine, q_near],
        [mine, near, above, across],
        [(parts, False)],
        pair + [("back", 2), ("pair", 2)],
        pair,
        SELF_TILE,
        "begin",
    )
    o_mine, o_theirs = attend(
        scalars,
        [q_mine, q_near],
        [far],
        [(parts, False)],
        [("odd", 2)],
        pair,
        SELF_TILE,
        "finish",
        [*state, o_mine, o_theirs],
    )
    both = lambda i: ((i // head) ^ 1) * head + ((i % head) ^ 2)
    route = [(i, both(i)) for i in range(seq * head)]
    corner = lax.ppermute(o_theirs, ("seq", "head"), route)
    flip = lambda i: i ^ 1
    places = jnp.stack([place, lane])
    contexts = [o_mine, send(o_theirs, "seq", swap), send(o_mine, "head", lambda i: i ^ 2), corner]
    others = [send(piece, "head", flip) for piece in contexts]
    (partial,) = project_call(
        places,
        residual,
        contexts[:2] + others[:2],
        [w_blocks[0], w_blocks[2]],
        True,
        jnp.float32,
    )
    hidden, hidden_low, hidden_high = project_call(
        places,
        partial,
        contexts[2:] + others[2:],
        [w_blocks[1], w_blocks[3]],
        False,
        jnp.bfloat16,
    )
    beside = lambda i: i ^ 2
    x_low = send(hidden_low, "head", beside)
    y_high = send(hidden_high, "seq", swap)
    x_high = send(hidden_high, "head", beside)
    y_low = send(hidden_low, "seq", swap)
    corner_low = send(x_low, "seq", swap)
    corner_high = send(y_high, "head", beside)
    own_core = send(hidden, "head", flip)
    core = [
        send(piece, "head", flip)
        for piece in (x_low, x_high, y_low, y_high, corner_low, corner_high)
    ]
    cut = rows // 2
    whole, low_rows, high_rows = slice(0, cut), slice(0, cut), slice(cut, rows)
    gain = norm_gain[None, :]
    groups = [
        (0, [(hidden, low_rows), (own_core, low_rows), (x_low, whole), (core[0], whole)]),
        (cut, [(hidden, high_rows), (own_core, high_rows), (x_high, whole), (core[1], whole)]),
    ]
    normed_mine, cache_mine = cache_call(place1, lane1, gain, groups, cache_pieces, rings)
    groups = [
        (0, [(a, whole) for a in (y_low, core[2], corner_low, core[4])]),
        (cut, [(a, whole) for a in (y_high, core[3], corner_high, core[5])]),
    ]
    normed_near, cache_near = cache_call(place1, lane1, gain, groups, cache_pieces, rings)
    q_pair = query_call(place1, [normed_mine, normed_near], query_pieces, rings)
    cache_above = send(cache_mine, "seq", up)
    cache_across = send(cache_near, "seq", up)
    cache_odd = jnp.where(side == 1, cache_above, cache_across)
    cache_far = send(cache_odd, "seq", up, lambda i: i >= 2)
    o_mine, o_theirs, *state = attend(
        scalars,
        q_pair,
        [cache_mine, cache_near, cache_above, cache_across],
        [(parts, True)],
        pair + [("back", 2), ("pair", 2)],
        pair,
        CROSS_TILE,
        "begin",
    )
    o_mine, o_theirs = attend(
        scalars,
        q_pair,
        [cache_far],
        [(parts, True)],
        [("odd", 2)],
        pair,
        CROSS_TILE,
        "finish",
        [*state, o_mine, o_theirs],
    )
    cross_context = ordered(o_mine, send(o_theirs, "seq", swap), 1)
    return (hidden, cross_context)


def direct_attend_kernel(
    place_ref, doc_ref, tail_ref, q_ref, *refs, slots, heads, group, q_tile, reach
):
    kv_refs = refs[: len(slots)]
    o_ref, m_ref, l_ref, acc_ref = refs[len(slots) :]
    rows = q_ref.shape[0]
    blocks = doc_ref.shape[0]
    kv_heads = heads // group
    factor = LOG2E / math.sqrt(HEAD_DIM)
    here = place_ref[0]
    own_doc = doc_ref[here]
    after = jnp.minimum(here + 1, blocks - 1)
    closing = jnp.logical_or(here == blocks - 1, doc_ref[after] != own_doc)
    live = jnp.where(closing, tail_ref[here], rows)

    def scores(kv_ref, t, h):
        q = q_ref[pl.ds(t, q_tile), h * HEAD_DIM : (h + 1) * HEAD_DIM]
        g = h // group
        k = kv_ref[:, g * HEAD_DIM : (g + 1) * HEAD_DIM]
        return lax.dot_general(q, k, (((1,), (1,)), ((), ())), preferred_element_type=jnp.float32)

    def values(kv_ref, h):
        g = kv_heads + h // group
        return kv_ref[:, g * HEAD_DIM : (g + 1) * HEAD_DIM]

    def tiles(step):
        def body(i, carry):
            step(pl.multiple_of(i * q_tile, q_tile))
            return carry

        lax.fori_loop(0, rows // q_tile, body, 0)

    def first(t):
        kv_ref = kv_refs[0]
        row = t + lax.broadcasted_iota(jnp.int32, (q_tile, rows), 0)
        col = lax.broadcasted_iota(jnp.int32, (q_tile, rows), 1)
        keep = jnp.logical_and(col <= row, col < live)
        for h in range(heads):
            s = jnp.where(keep, scores(kv_ref, t, h), -1e30)
            m = jnp.max(s, axis=1, keepdims=True)
            p = jnp.exp2((s - m) * factor)
            m_ref[h, pl.ds(t, q_tile), :] = jnp.broadcast_to(m, (q_tile, HEAD_DIM))
            l_ref[h, pl.ds(t, q_tile), :] = jnp.broadcast_to(
                jnp.sum(p, axis=1, keepdims=True), (q_tile, HEAD_DIM)
            )
            acc_ref[h, pl.ds(t, q_tile), :] = jnp.dot(
                p.astype(jnp.bfloat16), values(kv_ref, h), preferred_element_type=jnp.float32
            )

    def later(kv_ref, back):
        def step(t):
            if back * rows + rows - 1 >= reach:
                row = t + lax.broadcasted_iota(jnp.int32, (q_tile, rows), 0)
                col = lax.broadcasted_iota(jnp.int32, (q_tile, rows), 1)
                keep = back * rows + row - col < reach
            else:
                keep = None
            for h in range(heads):
                s = scores(kv_ref, t, h)
                if keep is not None:
                    s = jnp.where(keep, s, -1e30)
                m_old = m_ref[h, pl.ds(t, q_tile), :]
                m = jnp.maximum(m_old, jnp.max(s, axis=1, keepdims=True))
                shrink = jnp.exp2((m_old - m) * factor)
                p = jnp.exp2((s - m[:, :1]) * factor)
                m_ref[h, pl.ds(t, q_tile), :] = m
                l_ref[h, pl.ds(t, q_tile), :] = l_ref[h, pl.ds(t, q_tile), :] * shrink + jnp.sum(
                    p, axis=1, keepdims=True
                )
                acc_ref[h, pl.ds(t, q_tile), :] = acc_ref[
                    h, pl.ds(t, q_tile), :
                ] * shrink + jnp.dot(
                    p.astype(jnp.bfloat16), values(kv_ref, h), preferred_element_type=jnp.float32
                )

        return step

    tiles(first)
    for kv_ref, (even, odd) in zip(kv_refs[1:], slots[1:]):
        parity = lax.rem(here, 2)
        for back, only in ((even, 0), (odd, 1)):
            if back is None or (even == odd and only == 1):
                continue
            source = here - back
            wanted = jnp.logical_and(source >= 0, doc_ref[jnp.maximum(source, 0)] == own_doc)
            if even != odd:
                wanted = jnp.logical_and(wanted, parity == only)
            span = back

            @pl.when(wanted)
            def _(kv_ref=kv_ref, span=span):
                tiles(later(kv_ref, span))

    for h in range(heads):
        o_ref[:, h * HEAD_DIM : (h + 1) * HEAD_DIM] = (acc_ref[h] / l_ref[h]).astype(jnp.bfloat16)


def direct_attend(place, block_doc, tail_len, queries, column_block, heads, kv_list, slots, reach):
    rows, width = kv_list[0].shape
    kv_heads = width // (2 * HEAD_DIM)
    wide = heads * HEAD_DIM
    smem = pl.BlockSpec(memory_space=pltpu.SMEM)
    whole = pl.BlockSpec((rows, width), lambda i: (0, 0))
    return pl.pallas_call(
        functools.partial(
            direct_attend_kernel,
            slots=slots,
            heads=heads,
            group=heads // kv_heads,
            q_tile=min(256, rows),
            reach=reach,
        ),
        grid=(1,),
        out_shape=jax.ShapeDtypeStruct((rows, wide), jnp.bfloat16),
        in_specs=[smem, smem, smem, pl.BlockSpec((rows, wide), lambda i: (0, column_block))]
        + [whole] * len(kv_list),
        out_specs=pl.BlockSpec((rows, wide), lambda i: (0, 0)),
        scratch_shapes=[pltpu.VMEM((heads, rows, HEAD_DIM), jnp.float32)] * 3,
        compiler_params=pltpu.CompilerParams(vmem_limit_bytes=VMEM_LIMIT),
        name="attend",
    )(place, block_doc, tail_len, queries, *kv_list)


def direct_project_kernel(*refs, parts, blocks):
    residual_ref = refs[0]
    context_refs = refs[1 : 1 + parts * blocks]
    w_refs = refs[1 + parts * blocks : 1 + parts * blocks + blocks]
    o_ref = refs[-1]
    total = residual_ref[...].astype(jnp.float32)
    depth = context_refs[0].shape[1]
    for part in range(parts):
        for block in range(blocks):
            total += jnp.dot(
                context_refs[part * blocks + block][...],
                w_refs[block][part * depth : (part + 1) * depth, :],
                preferred_element_type=jnp.float32,
            )
    o_ref[...] = total.astype(jnp.bfloat16)


def norm_kernel(place_ref, gain_ref, *refs, near):
    hidden_refs, o_ref = refs[:-1], refs[-1]
    wide = hidden_refs[0].shape[1]
    total = 0.0
    for ref in hidden_refs:
        x = ref[...].astype(jnp.float32)
        total += jnp.sum(x * x, axis=1, keepdims=True)
    scale = lax.rsqrt(total / (wide * len(hidden_refs)) + EPSILON)
    for step, ref in enumerate(hidden_refs):
        at = pl.multiple_of(near(place_ref[0], step) * wide, wide)
        x = ref[...].astype(jnp.float32)
        o_ref[:, pl.ds(at, wide)] = (x * scale * gain_ref[:, pl.ds(at, wide)]).astype(jnp.bfloat16)


def columns_kernel(order_ref, normed_ref, *refs):
    w_refs, o_ref = refs[:-1], refs[-1]
    depth = w_refs[0].shape[0]
    total = 0.0
    for step, ref in enumerate(w_refs):
        at = pl.multiple_of(order_ref[step] * depth, depth)
        total += jnp.dot(
            normed_ref[:, pl.ds(at, depth)], ref[...], preferred_element_type=jnp.float32
        )
    o_ref[...] = total.astype(jnp.bfloat16)


def simple_call(kernel, out_shape, scalars, arrays):
    return pl.pallas_call(
        kernel,
        out_shape=out_shape,
        in_specs=[pl.BlockSpec(memory_space=pltpu.SMEM)] * len(scalars)
        + [pl.BlockSpec(memory_space=pltpu.VMEM)] * len(arrays),
        out_specs=pl.BlockSpec(memory_space=pltpu.VMEM),
        compiler_params=pltpu.CompilerParams(vmem_limit_bytes=VMEM_LIMIT),
    )(*scalars, *arrays)


def direct_layer(
    residual,
    q_self,
    k_self,
    v_self,
    w_out,
    norm_gain,
    w_query,
    w_cache,
    block_doc,
    tail_len,
    *,
    seq,
    head,
    span,
    paired,
):
    rows, own = residual.shape
    local_heads = q_self.shape[1] // HEAD_DIM
    place = lax.axis_index("seq").astype(jnp.int32)
    lane = lax.axis_index("head").astype(jnp.int32)
    place1, lane1 = place[None], lane[None]

    def along(block, target):
        return moved(block, "seq", seq, target)

    def across(block, step):
        return moved(block, "head", head, lambda i: i ^ step)

    even = lambda i: i % 2 == 0

    def spread(block):
        if not paired:
            return [along(block, lambda i, d=d: i + d) for d in range(1, span)]
        far = along(block, lambda i: i + 2)
        near = along(block, lambda i: i + 1 if even(i) else None)
        swap = along(far, lambda i: i ^ 1)
        last = along(swap, lambda i: i + 2 if even(i) else None)
        return [far, near, swap, last]

    if paired:
        slots = ((0, 0), (2, 2), (None, 1), (1, 3), (3, None))
    else:
        slots = tuple((d, d) for d in range(span))

    parts = local_heads // 2
    per = local_heads // parts
    width = per * HEAD_DIM
    kv_parts = []
    for c in range(parts):
        cols = slice(c * width, (c + 1) * width)
        own_kv = jnp.concatenate([k_self[:, cols], v_self[:, cols]], axis=1)
        kv_parts.append([own_kv] + spread(own_kv))

    w_blocks = []
    for step in range(head):
        piece = lax.dynamic_slice_in_dim(w_out, (lane ^ step) * own, own, 1)
        w_blocks.append(piece if step == 0 else across(piece, step))

    def gathered(w):
        if not paired:
            whole = lax.all_gather(w, "seq", axis=0, tiled=True)
            return [whole]
        pieces = [w, along(w, lambda i: i ^ 1)]
        ring = list(pieces)
        for distance in range(1, seq // 2):
            if distance <= seq // 4:
                ring = [along(p, lambda i: (i - 2) % seq) for p in ring]
                pieces += ring
            else:
                pieces += [
                    along(p, lambda i: (i + 2 * (seq // 2 - distance)) % seq) for p in pieces[:2]
                ]
        return pieces

    if paired:
        order = [(place ^ y) + 2 * distance for distance in range(seq // 2) for y in (0, 1)]
        order = jnp.stack([lax.rem(o, seq) for o in order])
    else:
        order = jnp.zeros((1,), jnp.int32)
    cache_w = gathered(w_cache)
    query_w = gathered(w_query)

    contexts = []
    for c in range(parts):
        mine = direct_attend(
            place1, block_doc, tail_len, q_self, c, per, kv_parts[c], slots, WINDOW
        )
        pair = [mine, across(mine, 2)]
        other = [across(p, 1) for p in pair]
        contexts += [pair[0], other[0], pair[1], other[1]]
    hidden = simple_call(
        functools.partial(direct_project_kernel, parts=parts, blocks=head),
        jax.ShapeDtypeStruct((rows, own), jnp.bfloat16),
        [],
        [residual, *contexts, *w_blocks],
    )
    pair = [hidden, across(hidden, 2)]
    other = [across(p, 1) for p in pair]
    normed = simple_call(
        functools.partial(norm_kernel, near=lambda at, step: at ^ step),
        jax.ShapeDtypeStruct((rows, own * head), jnp.bfloat16),
        [lane1],
        [norm_gain[None, :], pair[0], other[0], pair[1], other[1]],
    )
    cache = simple_call(
        columns_kernel,
        jax.ShapeDtypeStruct((rows, w_cache.shape[1]), jnp.bfloat16),
        [order],
        [normed, *cache_w],
    )
    history = [cache] + spread(cache)
    cross_queries = simple_call(
        columns_kernel,
        jax.ShapeDtypeStruct((rows, w_query.shape[1]), jnp.bfloat16),
        [order],
        [normed, *query_w],
    )
    cross_context = direct_attend(
        place1,
        block_doc,
        tail_len,
        cross_queries,
        0,
        local_heads,
        history,
        slots,
        rows * span,
    )
    return (hidden, cross_context)


def solution(mesh):
    seq, head = mesh.shape["seq"], mesh.shape["head"]
    span = min(5, seq // 2)
    in_specs = (
        P("seq", "head"),
        P("seq", "head"),
        P("seq", "head"),
        P("seq", "head"),
        P("head", None),
        P(),
        P("seq", "head"),
        P("seq", "head"),
        P(),
        P(),
    )
    out_specs = (P("seq", "head"), P("seq", "head"))
    if seq == 2 * span and head == 4:
        layer = functools.partial(paired_layer, seq=seq, head=head)
    else:
        layer = functools.partial(direct_layer, seq=seq, head=head, span=span, paired=False)

    def body(*args):
        return layer(*args)

    return jax.shard_map(body, mesh=mesh, in_specs=in_specs, out_specs=out_specs, check_vma=False)
```
